32 devices in a mesh: leaf: 8 (over z, y), top: 4 (over x, core).
Axes of the slice: x: 2, y: 2, z: 4, core: 2. Of those that a mesh axis runs over, the one named last changes fastest.
Arguments:
- charges: float32 [4, 16, 4096], P('top', None, 'leaf'), may hold values from -6 to 6
- leaf_basis: float32 [4, 64, 64, 64], P('top', 'leaf'), may hold values from -0.75 to 0.75
- near_blocks: float32 [4, 64, 3, 64, 64], P('top', 'leaf'), may hold values from -0.4375 to 0.4375
- near_list: int32 [4, 64, 3], P('top', 'leaf'), may hold values from 0 to 8
- local_transfer: float32 [4, 112, 64, 64], P('top', 'leaf'), may hold values from -0.5 to 0.5
- local_coupling: float32 [4, 112, 3, 64, 64], P('top', 'leaf'), may hold values from -0.4375 to 0.4375
- coupling_list: int32 [4, 112, 3], P('top', 'leaf'), may hold values from 0 to 23, as said below
- coarse_transfer: float32 [4, 3, 2, 64, 64], P('top'), may hold values from -0.5 to 0.5
- coarse_coupling: float32 [4, 1, 4, 64, 64], P('top'), may hold values from -0.4375 to 0.4375
- opposite_coupling: float32 [4, 64, 64], P('top'), may hold values from -0.75 to 0.75
- body_coupling: float32 [4, 3, 64, 64], P('top'), may hold values from -0.4375 to 0.4375
Outputs:
- potential: float32 [4, 16, 4096], P('top', None, 'leaf')
The draws below stay inside these ranges and needn't reach their ends.
Inputs may be any that keep to these rules, and one draw needn't show every extreme that they name: `coupling_list`: for a node of a device tier with m nodes per device the entry lies below 3 m; it names, in order, the m nodes of that tier on the previous device along the boundary, then this device's, then the next device's.
All inputs are finite; a program needn't handle non-finite values.
Results may differ from the reference program's by a relative error of at most 0.0001.
Values sent between devices are 32-bit elements; how exact they have to be, the bound alone decides.
No kernel may reach another device: no remote copies, remote signals or barrier semaphores. Data moves between devices by JAX's collectives and lax.ppermute only.
A program may use at most 64 MiB of HBM per device.

```python
import jax
import jax.numpy as jnp
import numpy as np
from jax import lax

K = 64
RHS = 16
P_SIZE = 64
L0 = 8
NEAR = 4
LEVELS = 3
COARSE = 3
NODES = 14
LEAVES = 64
N_LEAF = 8
N_TOP = 4


def draw_coupling_list(key, part):
    ranges = np.concatenate([np.full(L0 >> height, 3 * (L0 >> height)) for height in range(LEVELS)])
    limits = jnp.asarray(np.tile(ranges, N_LEAF), dtype=jnp.int32)
    return jax.random.randint(key, (N_TOP, N_LEAF * (2 * L0 - 2), 3), 0, limits[None, :, None], dtype=jnp.int32)


def set_ends(array, key, low, largest):
    extent = array.shape
    index_at = [jax.random.randint(jax.random.fold_in(key, axis), (), 0, extent[axis]) for axis in range(len(extent))]
    array = array.at[tuple(index_at)].set(low)
    longest = extent.index(max(extent))
    index_at[longest] = (index_at[longest] + 1) % extent[longest]
    return array.at[tuple(index_at)].set(largest)


def steps_of(key, dims, cuts, least, largest):
    factor_of = 1.0
    for axis_at, shards_of in cuts:
        steps = jax.random.uniform(jax.random.fold_in(jax.random.fold_in(key, 6), axis_at), (shards_of,), jnp.float32, least / len(cuts), largest / len(cuts))
        factor_of = factor_of * jnp.repeat(jnp.exp(steps), dims[axis_at] // shards_of).reshape((-1,) + (1,) * (len(dims) - 1 - axis_at))
    return factor_of


def bell_draw(own_key, extent, deviation, reach, shards=(), held_as=jnp.bfloat16):
    values = deviation * jax.random.normal(own_key, extent, jnp.float32)
    if shards:
        values = values * steps_of(own_key, extent, shards, -0.22, 0.18)
    return jnp.clip(values, -reach, reach).astype(held_as)


def setup_inputs(seed: int = 0) -> dict:
    key_list = jax.random.split(jax.random.key(seed), 12)
    return {
        "charges": bell_draw(key_list[0], (N_TOP, RHS, LEAVES * P_SIZE), 1.0, 6.0, ((0, 4), (2, 8)), jnp.float32),
        "leaf_basis": bell_draw(key_list[1], (N_TOP, LEAVES, P_SIZE, K), P_SIZE ** -0.5, 0.75, ((0, 4), (1, 8)), jnp.float32),
        "near_blocks": bell_draw(key_list[2], (N_TOP, LEAVES, 3, P_SIZE, P_SIZE), (3 * P_SIZE) ** -0.5, 0.4375, ((0, 4), (1, 8)), jnp.float32),
        "near_list": set_ends(jax.random.randint(key_list[3], (N_TOP, LEAVES, 3), 0, 2 * NEAR + 1), jax.random.fold_in(key_list[3], 1), 0, 2 * NEAR).astype(jnp.int32),
        "local_transfer": bell_draw(key_list[4], (N_TOP, N_LEAF * NODES, K, K), (2 * K) ** -0.5, 0.5, ((0, 4), (1, 8)), jnp.float32),
        "local_coupling": bell_draw(key_list[5], (N_TOP, N_LEAF * NODES, 3, K, K), (3 * K) ** -0.5, 0.4375, ((0, 4), (1, 8)), jnp.float32),
        "coupling_list": draw_coupling_list(jax.random.fold_in(key_list[11], 71), 0),
        "coarse_transfer": bell_draw(key_list[7], (N_TOP, COARSE, 2, K, K), (2 * K) ** -0.5, 0.5, ((0, 4),), jnp.float32),
        "coarse_coupling": bell_draw(key_list[8], (N_TOP, COARSE - 2, 4, K, K), (3 * K) ** -0.5, 0.4375, ((0, 4),), jnp.float32),
        "opposite_coupling": bell_draw(key_list[9], (N_TOP, K, K), K ** -0.5, 0.75, ((0, 4),), jnp.float32),
        "body_coupling": bell_draw(key_list[10], (N_TOP, N_TOP - 1, K, K), ((N_TOP - 1) * K) ** -0.5, 0.4375, ((0, 4),), jnp.float32),
    }


HIGH = lax.Precision.HIGHEST
OFFSETS = (-3, -2, 2, 3)


def upward(charges, leaf_basis, local_transfer):
    rhs = charges.shape[0]
    leaves = leaf_basis.shape[0]
    blocks = charges.reshape(rhs, leaves, P_SIZE)
    coeffs = [jnp.einsum('rnp,npk->rnk', blocks, leaf_basis, precision=HIGH)]
    nodes = local_transfer.reshape(N_LEAF, 2 * L0 - 2, K, K)
    for height in range(LEVELS):
        members = L0 >> height
        first = 2 * L0 - 2 * members
        mats = nodes[:, first:first + members].reshape(N_LEAF * members, K, K)
        moved = jnp.einsum('rnk,nkj->rnj', coeffs[-1], mats, precision=HIGH)
        coeffs.append(moved[:, 0::2] + moved[:, 1::2])
    return coeffs


def coarse_up(device_coeff, coarse_transfer):
    tiers = [device_coeff]
    for height in range(COARSE):
        below = tiers[-1]
        left = jnp.einsum('rnk,kj->rnj', below[:, 0::2], coarse_transfer[height, 0], precision=HIGH)
        right = jnp.einsum('rnk,kj->rnj', below[:, 1::2], coarse_transfer[height, 1], precision=HIGH)
        tiers.append(left + right)
    return tiers


def coarse_couple(tier, height, coarse_coupling, opposite_coupling):
    members = tier.shape[1]
    parity = jnp.arange(members, dtype=jnp.int32) % 2
    if height <= COARSE - 3:
        total = jnp.zeros_like(tier)
        for which, offset in enumerate(OFFSETS):
            moved = jnp.einsum('rnk,kj->rnj', jnp.roll(tier, -offset, axis=1), coarse_coupling[height, which], precision=HIGH)
            if offset == -3:
                keep = parity == 1
            elif offset == 3:
                keep = parity == 0
            else:
                keep = parity >= 0
            total = total + jnp.where(keep[None, :, None], moved, 0.0)
        return total
    if height == COARSE - 2:
        return jnp.einsum('rnk,kj->rnj', jnp.roll(tier, -2, axis=1), opposite_coupling, precision=HIGH)
    return jnp.zeros_like(tier)


def coarse_down(tiers, body_local, coarse_transfer, coarse_coupling, opposite_coupling):
    local = body_local
    for height in range(COARSE - 1, -1, -1):
        tier = tiers[height]
        members = tier.shape[1]
        parent = jnp.repeat(local, 2, axis=1)
        side = jnp.arange(members, dtype=jnp.int32) % 2
        mats = jnp.where(side[:, None, None] == 0, coarse_transfer[height, 0][None], coarse_transfer[height, 1][None])
        down = jnp.einsum('rnj,nkj->rnk', parent, mats, precision=HIGH)
        local = coarse_couple(tier, height, coarse_coupling, opposite_coupling) + down
    return local


def local_down(coeffs, device_local, local_transfer, local_coupling, coupling_list):
    nodes_t = local_transfer.reshape(N_LEAF, 2 * L0 - 2, K, K)
    nodes_s = local_coupling.reshape(N_LEAF, 2 * L0 - 2, 3, K, K)
    lists = coupling_list.reshape(N_LEAF, 2 * L0 - 2, 3)
    local = device_local
    for height in range(LEVELS - 1, -1, -1):
        members = L0 >> height
        first = 2 * L0 - 2 * members
        whole = N_LEAF * members
        window = lists[:, first:first + members]
        base = (jnp.arange(N_LEAF, dtype=jnp.int32) * members - members)[:, None, None]
        source = ((base + window) % whole).astype(jnp.int32).reshape(whole, 3)
        picked = coeffs[height][:, source]
        mats = nodes_s[:, first:first + members].reshape(whole, 3, K, K)
        coupled = jnp.einsum('rnsk,nskj->rnj', picked, mats, precision=HIGH)
        parent = jnp.repeat(local, 2, axis=1)
        trans = nodes_t[:, first:first + members].reshape(whole, K, K)
        down = jnp.einsum('rnj,nkj->rnk', parent, trans, precision=HIGH)
        local = coupled + down
    return local


def reference(charges, leaf_basis, near_blocks, near_list, local_transfer, local_coupling, coupling_list, coarse_transfer, coarse_coupling, opposite_coupling, body_coupling):
    ups = []
    tops = []
    for body_index in range(N_TOP):
        coeffs = upward(charges[body_index], leaf_basis[body_index], local_transfer[body_index])
        tiers = coarse_up(coeffs[-1], coarse_transfer[body_index])
        ups.append((coeffs, tiers))
        tops.append(tiers[-1])
    results = []
    for body_index in range(N_TOP):
        coeffs, tiers = ups[body_index]
        rhs = charges.shape[1]
        body_local = jnp.zeros((rhs, 1, K), jnp.float32)
        for which in range(N_TOP - 1):
            source = tops[(body_index + 1 + which) % N_TOP]
            body_local = body_local + jnp.einsum('rnk,kj->rnj', source, body_coupling[body_index, which], precision=HIGH)
        device_local = coarse_down(tiers, body_local, coarse_transfer[body_index], coarse_coupling[body_index], opposite_coupling[body_index])
        leaf_local = local_down(coeffs, device_local, local_transfer[body_index], local_coupling[body_index], coupling_list[body_index])
        far = jnp.einsum('rnk,npk->rnp', leaf_local, leaf_basis[body_index], precision=HIGH)
        blocks = charges[body_index].reshape(rhs, LEAVES, P_SIZE)
        source = ((jnp.arange(LEAVES, dtype=jnp.int32)[:, None] + near_list[body_index] - NEAR) % LEAVES).astype(jnp.int32)
        picked = blocks[:, source]
        near = jnp.einsum('rnsq,nsqp->rnp', picked, near_blocks[body_index], precision=HIGH)
        results.append((far + near).reshape(rhs, LEAVES * P_SIZE))
    return jnp.stack(results)
```

```python
import jax
import jax.numpy as jnp
from jax import lax
from jax.experimental import pallas as pl
from jax.experimental.pallas import tpu as pltpu
from jax.sharding import PartitionSpec as P

NEAR = 4
HIGH = lax.Precision.HIGH
VMEM = pltpu.MemorySpace.VMEM
SMEM = pltpu.MemorySpace.SMEM


def mm(a, b):
    return lax.dot_general(
        a, b, (((1,), (0,)), ((), ())), precision=HIGH, preferred_element_type=jnp.float32
    )


def mm_t(a, b):
    return lax.dot_general(
        a, b, (((1,), (1,)), ((), ())), precision=HIGH, preferred_element_type=jnp.float32
    )


def beside(a, b):
    return jnp.concatenate([a, b], axis=1)


def fold(x):
    half = x.shape[0] // 2
    return beside(x[:half], x[half:])


def unfold(x):
    half = x.shape[1] // 2
    return jnp.concatenate([x[:, :half], x[:, half:]], axis=0)


def tier_span(leaves, height):
    members = leaves >> height
    return 2 * leaves - 2 * members, members


def path_product(coarse_ref, position, tiers):
    product = None
    products = []
    for tier in range(tiers):
        matrix = coarse_ref[0, tier, (position >> tier) & 1]
        product = matrix if product is None else mm(product, matrix)
        products.append(product)
    return products


def up_kernel(charges, basis, transfer, coarse_transfer, ahead, behind, exchange):
    leaves, points = basis.shape[1], basis.shape[2]
    levels = leaves.bit_length() - 1
    position = lax.axis_index("leaf")
    body = lax.axis_index("top")
    top_count = exchange.shape[1]
    width = 2 * points
    reach = NEAR * points // width
    whole = leaves // 2
    pairs = leaves - 1
    for k in range(reach):
        first = (whole - reach + k) * width
        ahead[pairs + k] = charges[0, :, first : first + width]
        behind[pairs + k] = charges[0, :, k * width : (k + 1) * width]
    product = path_product(coarse_transfer, position, coarse_transfer.shape[1])[-1]
    coeffs = [mm(charges[0, :, g * points : (g + 1) * points], basis[0, g]) for g in range(leaves)]
    for height in range(levels):
        first, members = tier_span(leaves, height)
        for j in range(members // 2):
            pair = beside(coeffs[2 * j], coeffs[2 * j + 1])
            ahead[first // 2 + j] = pair
            behind[first // 2 + j] = pair
        coeffs = [
            mm(coeffs[2 * j], transfer[0, first + 2 * j])
            + mm(coeffs[2 * j + 1], transfer[0, first + 2 * j + 1])
            for j in range(members // 2)
        ]
    own = fold(coeffs[0])
    other = fold(mm(coeffs[0], product))
    for t in range(top_count):
        value = jnp.where(body == t, own, other)
        exchange[:, t] = jnp.broadcast_to(value[None], (exchange.shape[0],) + value.shape)


def middle_kernel(
    near_list,
    coupling_list,
    charges,
    basis,
    near_blocks,
    transfer,
    coupling,
    coarse_transfer,
    coarse_coupling,
    opposite,
    body_coupling,
    mine,
    below,
    above,
    known,
    mats,
    path,
    window,
    sources,
):
    leaves, points = basis.shape[1], basis.shape[2]
    rank = basis.shape[3]
    rhs = charges.shape[1]
    levels = leaves.bit_length() - 1
    position = lax.axis_index("leaf")
    coarse = coarse_transfer.shape[1]
    pairs = leaves - 1
    width = 2 * points
    reach = NEAR * points // width
    low_lanes = lax.broadcasted_iota(jnp.int32, (rhs, width), 1) < points

    def spread(pair, ref, even, odd):
        turned = pltpu.roll(pair, points, 1)
        ref[even] = jnp.where(low_lanes, pair, turned)
        ref[odd] = jnp.where(low_lanes, turned, pair)

    for k in range(reach):
        spread(below[pairs + k], sources, 2 * k, 2 * k + 1)
        at = NEAR + leaves + 2 * k
        spread(above[pairs + k], sources, at, at + 1)
    for k in range(leaves // 2):
        at = NEAR + 2 * k
        spread(charges[0, :, k * width : (k + 1) * width], sources, at, at + 1)
    for height in range(levels):
        first, members = tier_span(leaves, height)
        for block, pack in enumerate((below, mine, above)):
            for j in range(members // 2):
                at = 3 * first + block * members + 2 * j
                spread(pack[first // 2 + j], window, at, at + 1)

    def three(ref, base, list_ref, n):
        a = ref[base + list_ref[0, n, 0]]
        b = ref[base + list_ref[0, n, 1]]
        c = ref[base + list_ref[0, n, 2]]
        return beside(jnp.where(low_lanes, a, b), c[:, :points])

    near = []
    for g in range(leaves):
        left = three(sources, g, near_list, g)
        near.append(mm(left, near_blocks[0, g].reshape(3 * points, points)))
    local = None
    for height in range(levels - 1, -1, -1):
        first, members = tier_span(leaves, height)
        now = []
        for n in range(members):
            left = three(window, 3 * first, coupling_list, first + n)
            value = mm(left, coupling[0, first + n].reshape(3 * rank, rank))
            if local is not None:
                value = value + mm_t(local[n // 2], transfer[0, first + n])
            now.append(value)
        local = now
    for j in range(leaves // 2):
        value = [near[g] + mm_t(local[g], basis[0, g]) for g in (2 * j, 2 * j + 1)]
        known[:, j * width : (j + 1) * width] = beside(value[0], value[1])

    composite = None
    for height in range(levels - 1, -1, -1):
        first, members = tier_span(leaves, height)
        if composite is None:
            composite = [transfer[0, first + n] for n in range(members)]
        else:
            composite = [mm(transfer[0, first + n], composite[n // 2]) for n in range(members)]
    for g in range(leaves):
        path[g * points : (g + 1) * points] = mm(basis[0, g], composite[g])

    products = path_product(coarse_transfer, position, coarse)
    at = 0

    def put(value):
        nonlocal at
        mats[at : at + rank] = value
        at += rank

    for s in range(body_coupling.shape[1]):
        put(mm_t(body_coupling[0, s], products[coarse - 1]))
    for tier in range(coarse - 2):
        odd = (position >> tier) & 1
        for slot in (1, 2, jnp.where(odd == 1, 0, 3)):
            value = coarse_coupling[0, tier, slot]
            put(value if tier == 0 else mm_t(value, products[tier - 1]))
    far = mm_t(opposite[0], products[coarse - 3])
    put(mm(coarse_transfer[0, coarse - 3, 0], far))
    put(mm(coarse_transfer[0, coarse - 3, 1], far))


def final_kernel(received, known, mats, path, coarse_transfer, out, *tier_refs):
    leaf_count, top_count = received.shape[0], received.shape[1]
    coarse = coarse_transfer.shape[1]
    rhs = out.shape[1]
    position = lax.axis_index("leaf")
    body = lax.axis_index("top")
    terms = []
    for s in range(top_count - 1):
        other = lax.rem(body + 1 + s, top_count)
        total = received[0, other]
        for j in range(1, leaf_count):
            total = total + received[j, other]
        terms.append(unfold(total))

    def node(tier, index):
        if tier == 0:
            return unfold(received[index, body])
        return tier_refs[tier - 1][index]

    for tier in range(coarse - 2):
        count = leaf_count >> tier
        here = position >> tier
        odd = here & 1
        for offset in (-2, 2, jnp.where(odd == 1, -3, 3)):
            terms.append(node(tier, (here + offset + count) & (count - 1)))
        if tier < coarse - 3:
            for j in range(count // 2):
                tier_refs[tier][j] = mm(node(tier, 2 * j), coarse_transfer[0, tier, 0]) + mm(
                    node(tier, 2 * j + 1), coarse_transfer[0, tier, 1]
                )
    across = ((position >> (coarse - 2)) + 2) & 3
    terms.append(node(coarse - 3, 2 * across))
    terms.append(node(coarse - 3, 2 * across + 1))
    local = mm(jnp.concatenate(terms, axis=1), mats[...])
    out[0] = known[...] + mm_t(local, path[...])


def per_device(
    charges,
    leaf_basis,
    near_blocks,
    near_list,
    local_transfer,
    local_coupling,
    coupling_list,
    coarse_transfer,
    coarse_coupling,
    opposite_coupling,
    body_coupling,
):
    rhs = charges.shape[1]
    leaves, points, rank = leaf_basis.shape[1:]
    leaf_count = lax.axis_size("leaf")
    top_count = lax.axis_size("top")
    coarse = coarse_transfer.shape[1]
    packs = leaves - 1 + NEAR // 2
    f32 = jnp.float32
    vmem = pl.BlockSpec(memory_space=VMEM)
    smem = pl.BlockSpec(memory_space=SMEM)
    pack_shape = jax.ShapeDtypeStruct((packs, rhs, 2 * rank), f32)
    ahead, behind, exchange = pl.pallas_call(
        up_kernel,
        out_shape=(
            pack_shape,
            pack_shape,
            jax.ShapeDtypeStruct((leaf_count, top_count, rhs // 2, 2 * rank), f32),
        ),
        in_specs=[vmem] * 4,
        out_specs=(vmem,) * 3,
        name="up",
        cost_estimate=pl.CostEstimate(flops=40_000_000, bytes_accessed=1_000_000, transcendentals=0),
    )(charges, leaf_basis, local_transfer, coarse_transfer)
    forward = [(i, (i + 1) % leaf_count) for i in range(leaf_count)]
    backward = [(target, source) for source, target in forward]
    below = lax.ppermute(ahead, "leaf", forward)
    above = lax.ppermute(behind, "leaf", backward)
    received = lax.all_to_all(
        exchange.reshape(leaf_count * top_count, rhs // 2, 2 * rank),
        ("leaf", "top"),
        0,
        0,
        tiled=True,
    ).reshape(exchange.shape)
    terms = (top_count - 1) + 3 * (coarse - 2) + 2
    known, mats, path = pl.pallas_call(
        middle_kernel,
        out_shape=(
            jax.ShapeDtypeStruct((rhs, leaves * points), f32),
            jax.ShapeDtypeStruct((terms * rank, rank), f32),
            jax.ShapeDtypeStruct((leaves * points, rank), f32),
        ),
        in_specs=[smem] * 2 + [vmem] * 12,
        out_specs=(vmem,) * 3,
        scratch_shapes=[
            pltpu.VMEM((3 * (2 * leaves - 2), rhs, 2 * rank), f32),
            pltpu.VMEM((leaves + 2 * NEAR, rhs, 2 * points), f32),
        ],
        name="middle",
        cost_estimate=pl.CostEstimate(flops=80_000_000, bytes_accessed=3_000_000, transcendentals=0),
    )(
        near_list,
        coupling_list,
        charges,
        leaf_basis,
        near_blocks,
        local_transfer,
        local_coupling,
        coarse_transfer,
        coarse_coupling,
        opposite_coupling,
        body_coupling,
        ahead,
        below,
        above,
    )
    return pl.pallas_call(
        final_kernel,
        out_shape=jax.ShapeDtypeStruct(charges.shape, f32),
        in_specs=[vmem] * 5,
        out_specs=vmem,
        scratch_shapes=[
            pltpu.VMEM((leaf_count >> (tier + 1), rhs, rank), f32) for tier in range(coarse - 3)
        ],
        name="final",
        cost_estimate=pl.CostEstimate(flops=10_000_000, bytes_accessed=600_000, transcendentals=0),
    )(received, known, mats, path, coarse_transfer)


def solution(mesh):
    in_specs = (
        P("top", None, "leaf"),
        P("top", "leaf", None, None),
        P("top", "leaf", None, None, None),
        P("top", "leaf", None),
        P("top", "leaf", None, None),
        P("top", "leaf", None, None, None),
        P("top", "leaf", None),
        P("top", None, None, None, None),
        P("top", None, None, None, None),
        P("top", None, None),
        P("top", None, None, None),
    )
    out_specs = P("top", None, "leaf")
    return jax.shard_map(
        per_device, mesh=mesh, in_specs=in_specs, out_specs=out_specs, check_vma=False
    )
```

```python
import jax
import jax.numpy as jnp
from jax import lax
from jax.experimental import pallas as pl
from jax.experimental.pallas import tpu as pltpu
from jax.sharding import PartitionSpec as P

NEAR = 4
HIGH = lax.Precision.HIGH
VMEM = pltpu.MemorySpace.VMEM
SMEM = pltpu.MemorySpace.SMEM
HBM = pltpu.MemorySpace.HBM


def mm(a, b):
    return lax.dot_general(
        a, b, (((1,), (0,)), ((), ())), precision=HIGH, preferred_element_type=jnp.float32
    )


def mm_t(a, b):
    return lax.dot_general(
        a, b, (((1,), (1,)), ((), ())), precision=HIGH, preferred_element_type=jnp.float32
    )


def beside(a, b):
    return jnp.concatenate([a, b], axis=1)


def fold(x):
    half = x.shape[0] // 2
    return beside(x[:half], x[half:])


def unfold(x):
    half = x.shape[1] // 2
    return jnp.concatenate([x[:, :half], x[:, half:]], axis=0)


def tier_span(leaves, height):
    members = leaves >> height
    return 2 * leaves - 2 * members, members


def path_product(coarse_ref, position, tiers):
    product = None
    products = []
    for tier in range(tiers):
        matrix = coarse_ref[0, tier, (position >> tier) & 1]
        product = matrix if product is None else mm(product, matrix)
        products.append(product)
    return products


def fetch(sources, targets, sem):
    copies = [
        pltpu.make_async_copy(source, target, sem.at[i])
        for i, (source, target) in enumerate(zip(sources, targets))
    ]
    for copy in copies:
        copy.start()
    return copies


def up_kernel(
    charges_hbm,
    basis_hbm,
    transfer_hbm,
    coarse_hbm,
    ahead,
    behind,
    exchange,
    charges,
    basis,
    transfer,
    coarse_transfer,
    sem,
):
    copies = fetch(
        (charges_hbm, basis_hbm, coarse_hbm, transfer_hbm),
        (charges, basis, coarse_transfer, transfer),
        sem,
    )
    leaves, points = basis.shape[1], basis.shape[2]
    levels = leaves.bit_length() - 1
    position = lax.axis_index("leaf")
    body = lax.axis_index("top")
    top_count = exchange.shape[1]
    width = 2 * points
    reach = NEAR * points // width
    whole = leaves // 2
    pairs = leaves - 1
    copies[0].wait()
    copies[1].wait()
    for k in range(reach):
        first = (whole - reach + k) * width
        ahead[pairs + k] = charges[0, :, first : first + width]
        behind[pairs + k] = charges[0, :, k * width : (k + 1) * width]
    copies[2].wait()
    product = path_product(coarse_transfer, position, coarse_transfer.shape[1])[-1]
    copies[3].wait()
    coeffs = [mm(charges[0, :, g * points : (g + 1) * points], basis[0, g]) for g in range(leaves)]
    for height in range(levels):
        first, members = tier_span(leaves, height)
        for j in range(members // 2):
            pair = beside(coeffs[2 * j], coeffs[2 * j + 1])
            ahead[first // 2 + j] = pair
            behind[first // 2 + j] = pair
        coeffs = [
            mm(coeffs[2 * j], transfer[0, first + 2 * j])
            + mm(coeffs[2 * j + 1], transfer[0, first + 2 * j + 1])
            for j in range(members // 2)
        ]
    own = fold(coeffs[0])
    other = fold(mm(coeffs[0], product))
    for t in range(top_count):
        value = jnp.where(body == t, own, other)
        exchange[:, t] = jnp.broadcast_to(value[None], (exchange.shape[0],) + value.shape)


def prep_kernel(
    basis,
    transfer,
    coarse_transfer,
    coarse_coupling_hbm,
    opposite_hbm,
    body_coupling_hbm,
    near_hbm,
    coupling_hbm,
    mats,
    local_path,
    path,
    near_blocks,
    coupling,
    coarse_coupling,
    opposite,
    body_coupling,
    sem,
):
    copies = fetch(
        (coarse_coupling_hbm, opposite_hbm, body_coupling_hbm, near_hbm, coupling_hbm),
        (coarse_coupling, opposite, body_coupling, near_blocks, coupling),
        sem,
    )
    leaves, points, rank = basis.shape[1:]
    levels = leaves.bit_length() - 1
    position = lax.axis_index("leaf")
    coarse = coarse_transfer.shape[1]
    for g in range(leaves):
        product = basis[0, g]
        for height in range(levels):
            local_path[g, height * rank : (height + 1) * rank] = product.T
            first, _ = tier_span(leaves, height)
            product = mm(product, transfer[0, first + (g >> height)])
        path[g] = product.T

    products = path_product(coarse_transfer, position, coarse)
    at = 0

    def put(value):
        nonlocal at
        mats[at : at + rank] = value
        at += rank

    for copy in copies[:3]:
        copy.wait()
    for s in range(body_coupling.shape[1]):
        put(mm_t(body_coupling[0, s], products[coarse - 1]))
    for tier in range(coarse - 2):
        odd = (position >> tier) & 1
        for slot in (1, 2, jnp.where(odd == 1, 0, 3)):
            value = coarse_coupling[0, tier, slot]
            put(value if tier == 0 else mm_t(value, products[tier - 1]))
    far = mm_t(opposite[0], products[coarse - 3])
    put(mm(coarse_transfer[0, coarse - 3, 0], far))
    put(mm(coarse_transfer[0, coarse - 3, 1], far))
    for copy in copies[3:]:
        copy.wait()


def near_kernel(
    near_list,
    coupling_list,
    charges,
    near_blocks,
    coupling,
    local_path,
    mine,
    below,
    above,
    known,
    window,
    sources,
):
    leaves, points = near_blocks.shape[1], near_blocks.shape[3]
    rank = coupling.shape[3]
    rhs = charges.shape[1]
    levels = leaves.bit_length() - 1
    pairs = leaves - 1
    width = 2 * points
    reach = NEAR * points // width
    low_lanes = lax.broadcasted_iota(jnp.int32, (rhs, width), 1) < points

    def spread(pair, ref, even, odd):
        turned = pltpu.roll(pair, points, 1)
        ref[even] = jnp.where(low_lanes, pair, turned)
        ref[odd] = jnp.where(low_lanes, turned, pair)

    for k in range(reach):
        spread(below[pairs + k], sources, 2 * k, 2 * k + 1)
        at = NEAR + leaves + 2 * k
        spread(above[pairs + k], sources, at, at + 1)
    for k in range(leaves // 2):
        at = NEAR + 2 * k
        spread(charges[0, :, k * width : (k + 1) * width], sources, at, at + 1)
    for height in range(levels):
        first, members = tier_span(leaves, height)
        for block, pack in enumerate((below, mine, above)):
            for j in range(members // 2):
                at = 3 * first + block * members + 2 * j
                spread(pack[first // 2 + j], window, at, at + 1)

    def three(ref, base, list_ref, n):
        a = ref[base + list_ref[0, 0, n]]
        b = ref[base + list_ref[1, 0, n]]
        c = ref[base + list_ref[2, 0, n]]
        return beside(jnp.where(low_lanes, a, b), c[:, :points])

    coupled = []
    for n in range(2 * leaves - 2):
        height = next(h for h in range(levels) if n < sum(tier_span(leaves, h)))
        left = three(window, 3 * tier_span(leaves, height)[0], coupling_list, n)
        coupled.append(mm(left, coupling[0, n].reshape(3 * rank, rank)))
    result = []
    for g in range(leaves):
        left = three(sources, g, near_list, g)
        value = mm(left, near_blocks[0, g].reshape(3 * points, points))
        chain = [coupled[tier_span(leaves, h)[0] + (g >> h)] for h in range(levels)]
        result.append(value + mm(jnp.concatenate(chain, axis=1), local_path[g]))
    for j in range(leaves // 2):
        known[:, j * width : (j + 1) * width] = beside(result[2 * j], result[2 * j + 1])


def final_kernel(received, known, mats, path, coarse_transfer, out, *tier_refs):
    leaf_count, top_count = received.shape[0], received.shape[1]
    coarse = coarse_transfer.shape[1]
    rhs = out.shape[1]
    position = lax.axis_index("leaf")
    body = lax.axis_index("top")
    terms = []
    for s in range(top_count - 1):
        other = lax.rem(body + 1 + s, top_count)
        total = received[0, other]
        for j in range(1, leaf_count):
            total = total + received[j, other]
        terms.append(unfold(total))

    def node(tier, index):
        if tier == 0:
            return unfold(received[index, body])
        return tier_refs[tier - 1][index]

    for tier in range(coarse - 2):
        count = leaf_count >> tier
        here = position >> tier
        odd = here & 1
        for offset in (-2, 2, jnp.where(odd == 1, -3, 3)):
            terms.append(node(tier, (here + offset + count) & (count - 1)))
        if tier < coarse - 3:
            for j in range(count // 2):
                tier_refs[tier][j] = mm(node(tier, 2 * j), coarse_transfer[0, tier, 0]) + mm(
                    node(tier, 2 * j + 1), coarse_transfer[0, tier, 1]
                )
    across = ((position >> (coarse - 2)) + 2) & 3
    terms.append(node(coarse - 3, 2 * across))
    terms.append(node(coarse - 3, 2 * across + 1))
    local = mm(jnp.concatenate(terms, axis=1), mats[...])
    points = path.shape[2]
    for j in range(path.shape[0] // 2):
        at = 2 * j * points
        value = beside(mm(local, path[2 * j]), mm(local, path[2 * j + 1]))
        out[0, :, at : at + 2 * points] = known[:, at : at + 2 * points] + value


def per_device(
    charges,
    leaf_basis,
    near_blocks,
    near_list,
    local_transfer,
    local_coupling,
    coupling_list,
    coarse_transfer,
    coarse_coupling,
    opposite_coupling,
    body_coupling,
):
    rhs = charges.shape[1]
    leaves, points, rank = leaf_basis.shape[1:]
    leaf_count = lax.axis_size("leaf")
    top_count = lax.axis_size("top")
    coarse = coarse_transfer.shape[1]
    packs = leaves - 1 + NEAR // 2
    f32 = jnp.float32
    vmem = pl.BlockSpec(memory_space=VMEM)
    smem = pl.BlockSpec(memory_space=SMEM)
    params = pltpu.CompilerParams(vmem_limit_bytes=8 << 20)
    pack_shape = jax.ShapeDtypeStruct((packs, rhs, 2 * rank), f32)
    hbm = pl.BlockSpec(memory_space=HBM)

    def like(*arrays):
        return tuple(jax.ShapeDtypeStruct(array.shape, array.dtype) for array in arrays)

    def stay(*arrays):
        return [pltpu.with_memory_space_constraint(array, HBM) for array in arrays]

    ahead, behind, exchange, charges_v, basis_v, transfer_v, coarse_v = pl.pallas_call(
        up_kernel,
        out_shape=(
            pack_shape,
            pack_shape,
            jax.ShapeDtypeStruct((leaf_count, top_count, rhs // 2, 2 * rank), f32),
        )
        + like(charges, leaf_basis, local_transfer, coarse_transfer),
        in_specs=[hbm] * 4,
        out_specs=(vmem,) * 7,
        scratch_shapes=[pltpu.SemaphoreType.DMA((4,))],
        name="up",
        compiler_params=params,
        cost_estimate=pl.CostEstimate(flops=40_000_000, bytes_accessed=1_000_000, transcendentals=0),
    )(*stay(charges, leaf_basis, local_transfer, coarse_transfer))
    forward = [(i, (i + 1) % leaf_count) for i in range(leaf_count)]
    backward = [(target, source) for source, target in forward]
    below = lax.ppermute(ahead, "leaf", forward)
    above = lax.ppermute(behind, "leaf", backward)
    received = lax.all_to_all(
        exchange.reshape(leaf_count * top_count, rhs // 2, 2 * rank),
        ("leaf", "top"),
        0,
        0,
        tiled=True,
    ).reshape(exchange.shape)
    terms = (top_count - 1) + 3 * (coarse - 2) + 2
    levels = leaves.bit_length() - 1
    mats, local_path, path, near_v, coupling_v = pl.pallas_call(
        prep_kernel,
        out_shape=(
            jax.ShapeDtypeStruct((terms * rank, rank), f32),
            jax.ShapeDtypeStruct((leaves, levels * rank, points), f32),
            jax.ShapeDtypeStruct((leaves, rank, points), f32),
        )
        + like(near_blocks, local_coupling),
        in_specs=[vmem] * 3 + [hbm] * 5,
        out_specs=(vmem,) * 5,
        scratch_shapes=[
            pltpu.VMEM(array.shape, f32)
            for array in (coarse_coupling, opposite_coupling, body_coupling)
        ]
        + [pltpu.SemaphoreType.DMA((5,))],
        name="prep",
        compiler_params=params,
        cost_estimate=pl.CostEstimate(flops=40_000_000, bytes_accessed=2_000_000, transcendentals=0),
    )(
        basis_v,
        transfer_v,
        coarse_v,
        *stay(coarse_coupling, opposite_coupling, body_coupling, near_blocks, local_coupling),
    )
    known = pl.pallas_call(
        near_kernel,
        out_shape=jax.ShapeDtypeStruct((rhs, leaves * points), f32),
        in_specs=[smem] * 2 + [vmem] * 7,
        out_specs=vmem,
        scratch_shapes=[
            pltpu.VMEM((3 * (2 * leaves - 2), rhs, 2 * rank), f32),
            pltpu.VMEM((leaves + 2 * NEAR, rhs, 2 * points), f32),
        ],
        name="near",
        compiler_params=params,
        cost_estimate=pl.CostEstimate(flops=80_000_000, bytes_accessed=3_000_000, transcendentals=0),
    )(
        jnp.transpose(near_list, (2, 0, 1)),
        jnp.transpose(coupling_list, (2, 0, 1)),
        charges_v,
        near_v,
        coupling_v,
        local_path,
        ahead,
        below,
        above,
    )
    return pl.pallas_call(
        final_kernel,
        out_shape=jax.ShapeDtypeStruct(charges.shape, f32),
        in_specs=[vmem] * 5,
        out_specs=vmem,
        scratch_shapes=[
            pltpu.VMEM((leaf_count >> (tier + 1), rhs, rank), f32) for tier in range(coarse - 3)
        ],
        name="final",
        compiler_params=params,
        cost_estimate=pl.CostEstimate(flops=10_000_000, bytes_accessed=600_000, transcendentals=0),
    )(received, known, mats, path, coarse_v)


def solution(mesh):
    in_specs = (
        P("top", None, "leaf"),
        P("top", "leaf", None, None),
        P("top", "leaf", None, None, None),
        P("top", "leaf", None),
        P("top", "leaf", None, None),
        P("top", "leaf", None, None, None),
        P("top", "leaf", None),
        P("top", None, None, None, None),
        P("top", None, None, None, None),
        P("top", None, None),
        P("top", None, None, None),
    )
    out_specs = P("top", None, "leaf")
    return jax.shard_map(
        per_device, mesh=mesh, in_specs=in_specs, out_specs=out_specs, check_vma=False
    )
```

```python
import jax
import jax.numpy as jnp
from jax import lax
from jax.experimental import pallas as pl
from jax.experimental.pallas import tpu as pltpu
from jax.sharding import PartitionSpec as P

NEAR = 4
HIGH = lax.Precision.HIGH
VMEM = pltpu.MemorySpace.VMEM
SMEM = pltpu.MemorySpace.SMEM
HBM = pltpu.MemorySpace.HBM


def mm(a, b):
    return lax.dot_general(
        a, b, (((1,), (0,)), ((), ())), precision=HIGH, preferred_element_type=jnp.float32
    )


def mm_t(a, b):
    return lax.dot_general(
        a, b, (((1,), (1,)), ((), ())), precision=HIGH, preferred_element_type=jnp.float32
    )


def beside(a, b):
    return jnp.concatenate([a, b], axis=1)


def fold(x):
    half = x.shape[0] // 2
    return beside(x[:half], x[half:])


def unfold(x):
    half = x.shape[1] // 2
    return jnp.concatenate([x[:, :half], x[:, half:]], axis=0)


def tier_span(leaves, height):
    members = leaves >> height
    return 2 * leaves - 2 * members, members


def path_product(coarse_ref, position, tiers):
    product = None
    products = []
    for tier in range(tiers):
        matrix = coarse_ref[0, tier, (position >> tier) & 1]
        product = matrix if product is None else mm(product, matrix)
        products.append(product)
    return products


def fetch(sources, targets, sem):
    copies = [
        pltpu.make_async_copy(source, target, sem.at[i])
        for i, (source, target) in enumerate(zip(sources, targets))
    ]
    for copy in copies:
        copy.start()
    return copies


def up_kernel(
    charges_hbm,
    basis_hbm,
    transfer_hbm,
    coarse_hbm,
    inner,
    outer,
    exchange,
    charges,
    basis,
    transfer,
    coarse_transfer,
    sem,
):
    copies = fetch(
        (charges_hbm, basis_hbm, coarse_hbm, transfer_hbm),
        (charges, basis, coarse_transfer, transfer),
        sem,
    )
    leaves, points = basis.shape[1], basis.shape[2]
    levels = leaves.bit_length() - 1
    position = lax.axis_index("leaf")
    body = lax.axis_index("top")
    top_count = exchange.shape[0]
    width = 2 * points
    reach = NEAR * points // width
    whole = leaves // 2
    pairs = leaves - 1
    copies[0].wait()
    copies[1].wait()
    odd = (position & 1) == 1
    for k in range(reach):
        first = (whole - reach + k) * width
        high = charges[0, :, first : first + width]
        low = charges[0, :, k * width : (k + 1) * width]
        inner[pairs + k] = jnp.where(odd, low, high)
        outer[pairs + k] = jnp.where(odd, high, low)
    copies[2].wait()
    product = path_product(coarse_transfer, position, coarse_transfer.shape[1])[-1]
    copies[3].wait()
    coeffs = [mm(charges[0, :, g * points : (g + 1) * points], basis[0, g]) for g in range(leaves)]
    for height in range(levels):
        first, members = tier_span(leaves, height)
        for j in range(members // 2):
            pair = beside(coeffs[2 * j], coeffs[2 * j + 1])
            inner[first // 2 + j] = pair
            outer[first // 2 + j] = pair
        coeffs = [
            mm(coeffs[2 * j], transfer[0, first + 2 * j])
            + mm(coeffs[2 * j + 1], transfer[0, first + 2 * j + 1])
            for j in range(members // 2)
        ]
    own = fold(coeffs[0])
    other = fold(mm(coeffs[0], product))
    for t in range(top_count):
        value = jnp.where(body == t, own, other)
        exchange[t] = jnp.broadcast_to(value[None], (exchange.shape[1],) + value.shape)


def prep_kernel(
    basis,
    transfer,
    coarse_transfer,
    coarse_coupling_hbm,
    opposite_hbm,
    body_coupling_hbm,
    near_hbm,
    coupling_hbm,
    mats,
    local_path,
    path,
    near_blocks,
    coupling,
    coarse_coupling,
    opposite,
    body_coupling,
    sem,
):
    copies = fetch(
        (coarse_coupling_hbm, opposite_hbm, body_coupling_hbm, near_hbm, coupling_hbm),
        (coarse_coupling, opposite, body_coupling, near_blocks, coupling),
        sem,
    )
    leaves, _, rank = basis.shape[1:]
    levels = leaves.bit_length() - 1
    position = lax.axis_index("leaf")
    coarse = coarse_transfer.shape[1]
    for g in range(leaves):
        product = basis[0, g]
        for height in range(levels):
            local_path[g, height * rank : (height + 1) * rank] = product.T
            first, _ = tier_span(leaves, height)
            product = mm(product, transfer[0, first + (g >> height)])
        path[g] = product.T

    products = path_product(coarse_transfer, position, coarse)
    at = 0

    def put(value):
        nonlocal at
        mats[at : at + rank] = value
        at += rank

    for copy in copies[:3]:
        copy.wait()
    for s in range(body_coupling.shape[1]):
        put(mm_t(body_coupling[0, s], products[coarse - 1]))
    for tier in range(coarse - 2):
        odd = (position >> tier) & 1
        for slot in (1, 2, jnp.where(odd == 1, 0, 3)):
            value = coarse_coupling[0, tier, slot]
            put(value if tier == 0 else mm_t(value, products[tier - 1]))
    far = mm_t(opposite[0], products[coarse - 3])
    put(mm(coarse_transfer[0, coarse - 3, 0], far))
    put(mm(coarse_transfer[0, coarse - 3, 1], far))
    for copy in copies[3:]:
        copy.wait()


def near_kernel(
    near_list,
    coupling_list,
    charges,
    near_blocks,
    coupling,
    local_path,
    mine,
    from_inner,
    from_outer,
    known,
    window,
    sources,
):
    leaves, points = near_blocks.shape[1], near_blocks.shape[3]
    rank = coupling.shape[3]
    rhs = charges.shape[1]
    levels = leaves.bit_length() - 1
    pairs = leaves - 1
    width = 2 * points
    reach = NEAR * points // width
    low_lanes = lax.broadcasted_iota(jnp.int32, (rhs, width), 1) < points

    def spread(pair, ref, even, odd):
        turned = pltpu.roll(pair, points, 1)
        ref[even] = jnp.where(low_lanes, pair, turned)
        ref[odd] = jnp.where(low_lanes, turned, pair)

    odd = lax.axis_index("leaf") & 1
    for k in range(reach):
        at = (1 - odd) * (NEAR + leaves) + 2 * k
        spread(from_inner[pairs + k], sources, at, at + 1)
        at = odd * (NEAR + leaves) + 2 * k
        spread(from_outer[pairs + k], sources, at, at + 1)
    for k in range(leaves // 2):
        at = NEAR + 2 * k
        spread(charges[0, :, k * width : (k + 1) * width], sources, at, at + 1)
    for height in range(levels):
        first, members = tier_span(leaves, height)
        for block, pack in ((2 - 2 * odd, from_inner), (1, mine), (2 * odd, from_outer)):
            for j in range(members // 2):
                at = 3 * first + block * members + 2 * j
                spread(pack[first // 2 + j], window, at, at + 1)

    def three(ref, base, list_ref, n):
        a = ref[base + list_ref[0, 0, n]]
        b = ref[base + list_ref[1, 0, n]]
        c = ref[base + list_ref[2, 0, n]]
        return beside(jnp.where(low_lanes, a, b), c[:, :points])

    coupled = []
    for n in range(2 * leaves - 2):
        height = next(h for h in range(levels) if n < sum(tier_span(leaves, h)))
        left = three(window, 3 * tier_span(leaves, height)[0], coupling_list, n)
        coupled.append(mm(left, coupling[0, n].reshape(3 * rank, rank)))
    result = []
    for g in range(leaves):
        left = three(sources, g, near_list, g)
        value = mm(left, near_blocks[0, g].reshape(3 * points, points))
        chain = [coupled[tier_span(leaves, h)[0] + (g >> h)] for h in range(levels)]
        result.append(value + mm(jnp.concatenate(chain, axis=1), local_path[g]))
    for j in range(leaves // 2):
        known[:, j * width : (j + 1) * width] = beside(result[2 * j], result[2 * j + 1])


def final_kernel(received, known, mats, path, coarse_transfer, out, *tier_refs):
    top_count, leaf_count = received.shape[0], received.shape[1]
    coarse = coarse_transfer.shape[1]
    position = lax.axis_index("leaf")
    body = lax.axis_index("top")
    terms = []
    for s in range(top_count - 1):
        other = lax.rem(body + 1 + s, top_count)
        total = received[other, 0]
        for j in range(1, leaf_count):
            total = total + received[other, j]
        terms.append(unfold(total))

    def node(tier, index):
        if tier == 0:
            return unfold(received[body, index])
        return tier_refs[tier - 1][index]

    for tier in range(coarse - 2):
        count = leaf_count >> tier
        here = position >> tier
        odd = here & 1
        for offset in (-2, 2, jnp.where(odd == 1, -3, 3)):
            terms.append(node(tier, (here + offset + count) & (count - 1)))
        if tier < coarse - 3:
            for j in range(count // 2):
                tier_refs[tier][j] = mm(node(tier, 2 * j), coarse_transfer[0, tier, 0]) + mm(
                    node(tier, 2 * j + 1), coarse_transfer[0, tier, 1]
                )
    across = ((position >> (coarse - 2)) + 2) & 3
    terms.append(node(coarse - 3, 2 * across))
    terms.append(node(coarse - 3, 2 * across + 1))
    local = mm(jnp.concatenate(terms, axis=1), mats[...])
    points = path.shape[2]
    for j in range(path.shape[0] // 2):
        at = 2 * j * points
        value = beside(mm(local, path[2 * j]), mm(local, path[2 * j + 1]))
        out[0, :, at : at + 2 * points] = known[:, at : at + 2 * points] + value


def per_device(
    charges,
    leaf_basis,
    near_blocks,
    near_list,
    local_transfer,
    local_coupling,
    coupling_list,
    coarse_transfer,
    coarse_coupling,
    opposite_coupling,
    body_coupling,
):
    rhs = charges.shape[1]
    leaves, points, rank = leaf_basis.shape[1:]
    leaf_count = lax.axis_size("leaf")
    top_count = lax.axis_size("top")
    coarse = coarse_transfer.shape[1]
    packs = leaves - 1 + NEAR // 2
    f32 = jnp.float32
    vmem = pl.BlockSpec(memory_space=VMEM)
    smem = pl.BlockSpec(memory_space=SMEM)
    params = pltpu.CompilerParams(vmem_limit_bytes=8 << 20)
    pack_shape = jax.ShapeDtypeStruct((packs, rhs, 2 * rank), f32)
    hbm = pl.BlockSpec(memory_space=HBM)

    def like(*arrays):
        return tuple(jax.ShapeDtypeStruct(array.shape, array.dtype) for array in arrays)

    def stay(*arrays):
        return [pltpu.with_memory_space_constraint(array, HBM) for array in arrays]

    inner, outer, exchange, charges_v, basis_v, transfer_v, coarse_v = pl.pallas_call(
        up_kernel,
        out_shape=(
            pack_shape,
            pack_shape,
            jax.ShapeDtypeStruct((top_count, leaf_count, rhs // 2, 2 * rank), f32),
        )
        + like(charges, leaf_basis, local_transfer, coarse_transfer),
        in_specs=[hbm] * 4,
        out_specs=(vmem,) * 7,
        scratch_shapes=[pltpu.SemaphoreType.DMA((4,))],
        name="up",
        compiler_params=params,
        cost_estimate=pl.CostEstimate(flops=40_000_000, bytes_accessed=1_000_000, transcendentals=0),
    )(*stay(charges, leaf_basis, local_transfer, coarse_transfer))
    inner_pairs = [(i, i ^ 1) for i in range(leaf_count)]
    outer_pairs = [(i, (i + (1 if i & 1 else -1)) % leaf_count) for i in range(leaf_count)]
    from_inner = lax.ppermute(inner, "leaf", inner_pairs)
    from_outer = lax.ppermute(outer, "leaf", outer_pairs)
    received = lax.all_to_all(
        exchange.reshape(leaf_count * top_count, rhs // 2, 2 * rank),
        ("top", "leaf"),
        0,
        0,
        tiled=True,
    ).reshape(exchange.shape)
    terms = (top_count - 1) + 3 * (coarse - 2) + 2
    levels = leaves.bit_length() - 1
    mats, local_path, path, near_v, coupling_v = pl.pallas_call(
        prep_kernel,
        out_shape=(
            jax.ShapeDtypeStruct((terms * rank, rank), f32),
            jax.ShapeDtypeStruct((leaves, levels * rank, points), f32),
            jax.ShapeDtypeStruct((leaves, rank, points), f32),
        )
        + like(near_blocks, local_coupling),
        in_specs=[vmem] * 3 + [hbm] * 5,
        out_specs=(vmem,) * 5,
        scratch_shapes=[
            pltpu.VMEM(array.shape, f32)
            for array in (coarse_coupling, opposite_coupling, body_coupling)
        ]
        + [pltpu.SemaphoreType.DMA((5,))],
        name="prep",
        compiler_params=params,
        cost_estimate=pl.CostEstimate(flops=40_000_000, bytes_accessed=2_000_000, transcendentals=0),
    )(
        basis_v,
        transfer_v,
        coarse_v,
        *stay(coarse_coupling, opposite_coupling, body_coupling, near_blocks, local_coupling),
    )
    known = pl.pallas_call(
        near_kernel,
        out_shape=jax.ShapeDtypeStruct((rhs, leaves * points), f32),
        in_specs=[smem] * 2 + [vmem] * 7,
        out_specs=vmem,
        scratch_shapes=[
            pltpu.VMEM((3 * (2 * leaves - 2), rhs, 2 * rank), f32),
            pltpu.VMEM((leaves + 2 * NEAR, rhs, 2 * points), f32),
        ],
        name="near",
        compiler_params=params,
        cost_estimate=pl.CostEstimate(flops=80_000_000, bytes_accessed=3_000_000, transcendentals=0),
    )(
        jnp.transpose(near_list, (2, 0, 1)),
        jnp.transpose(coupling_list, (2, 0, 1)),
        charges_v,
        near_v,
        coupling_v,
        local_path,
        inner,
        from_inner,
        from_outer,
    )
    return pl.pallas_call(
        final_kernel,
        out_shape=jax.ShapeDtypeStruct(charges.shape, f32),
        in_specs=[vmem] * 5,
        out_specs=vmem,
        scratch_shapes=[
            pltpu.VMEM((leaf_count >> (tier + 1), rhs, rank), f32) for tier in range(coarse - 3)
        ],
        name="final",
        compiler_params=params,
        cost_estimate=pl.CostEstimate(flops=10_000_000, bytes_accessed=600_000, transcendentals=0),
    )(received, known, mats, path, coarse_v)


def solution(mesh):
    in_specs = (
        P("top", None, "leaf"),
        P("top", "leaf", None, None),
        P("top", "leaf", None, None, None),
        P("top", "leaf", None),
        P("top", "leaf", None, None),
        P("top", "leaf", None, None, None),
        P("top", "leaf", None),
        P("top", None, None, None, None),
        P("top", None, None, None, None),
        P("top", None, None),
        P("top", None, None, None),
    )
    out_specs = P("top", None, "leaf")
    return jax.shard_map(
        per_device, mesh=mesh, in_specs=in_specs, out_specs=out_specs, check_vma=False
    )
```

```python
import jax
import jax.numpy as jnp
from jax import lax
from jax.experimental import pallas as pl
from jax.experimental.pallas import tpu as pltpu
from jax.sharding import PartitionSpec as P

NEAR = 4
HIGH = lax.Precision.HIGH
VMEM = pltpu.MemorySpace.VMEM
SMEM = pltpu.MemorySpace.SMEM
HBM = pltpu.MemorySpace.HBM


def mm(a, b):
    return lax.dot_general(
        a, b, (((1,), (0,)), ((), ())), precision=HIGH, preferred_element_type=jnp.float32
    )


def mm_t(a, b):
    return lax.dot_general(
        a, b, (((1,), (1,)), ((), ())), precision=HIGH, preferred_element_type=jnp.float32
    )


def halves(x):
    high = x.astype(jnp.bfloat16)
    return high, (x - high.astype(jnp.float32)).astype(jnp.bfloat16)


def packed(x):
    high = x.astype(jnp.bfloat16).astype(jnp.float32)
    return beside(high, x - high).astype(jnp.bfloat16)


def stacked(x):
    high, low = halves(x)
    return jnp.concatenate([high, low], axis=0)


def mm_s(a, b):
    rows = a.shape[0]
    left = stacked(a)
    high, low = halves(b)
    value = dot(left, high)
    return value[:rhs_of(value)] + value[rhs_of(value):] + dot(left[:rows], low)


def rhs_of(value):
    return value.shape[0] // 2


def dot(a, b):
    return lax.dot_general(a, b, (((1,), (0,)), ((), ())), preferred_element_type=jnp.float32)


def beside(a, b):
    return jnp.concatenate([a, b], axis=1)


def fold(x):
    half = x.shape[0] // 2
    return beside(x[:half], x[half:])


def unfold(x):
    half = x.shape[1] // 2
    return jnp.concatenate([x[:, :half], x[:, half:]], axis=0)


def tier_span(leaves, height):
    members = leaves >> height
    return 2 * leaves - 2 * members, members


def path_product(coarse_ref, position, tiers):
    product = None
    products = []
    for tier in range(tiers):
        matrix = coarse_ref[0, tier, (position >> tier) & 1]
        product = matrix if product is None else mm(product, matrix)
        products.append(product)
    return products


def fetch(sources, targets, sem):
    copies = [
        pltpu.make_async_copy(source, target, sem.at[i])
        for i, (source, target) in enumerate(zip(sources, targets))
    ]
    for copy in copies:
        copy.start()
    return copies


def up_kernel(
    charges_hbm,
    basis_hbm,
    transfer_hbm,
    coarse_hbm,
    coupling_hbm,
    inner,
    outer,
    exchange,
    charges,
    basis,
    transfer,
    coarse_transfer,
    coupling,
    sem,
):
    copies = fetch(
        (charges_hbm, basis_hbm, coarse_hbm, transfer_hbm, coupling_hbm),
        (charges, basis, coarse_transfer, transfer, coupling),
        sem,
    )
    leaves, points = basis.shape[1], basis.shape[2]
    levels = leaves.bit_length() - 1
    position = lax.axis_index("leaf")
    body = lax.axis_index("top")
    top_count = exchange.shape[0]
    width = 2 * points
    reach = NEAR * points // width
    whole = leaves // 2
    pairs = leaves - 1
    copies[0].wait()
    copies[1].wait()
    odd = (position & 1) == 1
    for k in range(reach):
        first = (whole - reach + k) * width
        high = charges[0, :, first : first + width]
        low = charges[0, :, k * width : (k + 1) * width]
        inner[pairs + k] = jnp.where(odd, low, high)
        outer[pairs + k] = jnp.where(odd, high, low)
    coeffs = [mm_s(charges[0, :, g * points : (g + 1) * points], basis[0, g]) for g in range(leaves)]
    copies[2].wait()
    copies[3].wait()
    tiers = coarse_transfer.shape[1]
    first, members = tier_span(leaves, levels - 1)
    steps = [coarse_transfer[0, tier, (position >> tier) & 1] for tier in range(tiers)]
    ends = [mm(transfer[0, first + n], steps[0]) for n in range(members)]
    rest = None
    for step in steps[:0:-1]:
        rest = step if rest is None else mm(step, rest)
    ends = [mm(end, rest) for end in ends]
    for height in range(levels):
        first, members = tier_span(leaves, height)
        for j in range(members // 2):
            pair = beside(coeffs[2 * j], coeffs[2 * j + 1])
            inner[first // 2 + j] = pair
            outer[first // 2 + j] = pair
        below = coeffs
        coeffs = [
            mm_s(below[2 * j], transfer[0, first + 2 * j])
            + mm_s(below[2 * j + 1], transfer[0, first + 2 * j + 1])
            for j in range(members // 2)
        ]
    own = fold(coeffs[0])
    other = fold(mm_s(below[0], ends[0]) + mm_s(below[1], ends[1]))
    for t in range(top_count):
        value = jnp.where(body == t, own, other)
        exchange[t] = jnp.broadcast_to(value[None], (exchange.shape[1],) + value.shape)
    copies[4].wait()


def prep_kernel(
    basis,
    transfer,
    coarse_transfer,
    coupling,
    coarse_coupling_hbm,
    opposite_hbm,
    body_coupling_hbm,
    near_hbm,
    mats,
    path,
    local_path,
    near_pack,
    coupling_pack,
    coarse_coupling,
    opposite,
    body_coupling,
    near_blocks,
    sem,
):
    copies = fetch(
        (coarse_coupling_hbm, opposite_hbm, body_coupling_hbm, near_hbm),
        (coarse_coupling, opposite, body_coupling, near_blocks),
        sem,
    )
    leaves, points, rank = basis.shape[1:]
    levels = leaves.bit_length() - 1
    position = lax.axis_index("leaf")
    coarse = coarse_transfer.shape[1]
    ends = []
    for g in range(leaves):
        product = basis[0, g]
        for height in range(levels):
            local_path[g, height * rank : (height + 1) * rank] = packed(product.T)
            first, _ = tier_span(leaves, height)
            product = mm(product, transfer[0, first + (g >> height)])
        ends.append(product.T)
    for j in range(leaves // 2):
        columns = slice(2 * j * points, 2 * (j + 1) * points)
        path[0, :, columns], path[1, :, columns] = halves(beside(ends[2 * j], ends[2 * j + 1]))
    for n in range(2 * leaves - 2):
        coupling_pack[n] = packed(coupling[0, n].reshape(3 * rank, rank))

    products = path_product(coarse_transfer, position, coarse)
    at = 0

    def put(value):
        nonlocal at
        rows = slice(at, at + rank)
        mats[0, rows], mats[1, rows] = halves(value)
        at += rank

    for copy in copies[:3]:
        copy.wait()
    for s in range(body_coupling.shape[1]):
        put(mm_t(body_coupling[0, s], products[coarse - 1]))
    for tier in range(coarse - 2):
        odd = (position >> tier) & 1
        for slot in (1, 2, jnp.where(odd == 1, 0, 3)):
            value = coarse_coupling[0, tier, slot]
            put(value if tier == 0 else mm_t(value, products[tier - 1]))
    far = mm_t(opposite[0], products[coarse - 3])
    put(mm(coarse_transfer[0, coarse - 3, 0], far))
    put(mm(coarse_transfer[0, coarse - 3, 1], far))
    copies[3].wait()
    for g in range(leaves):
        near_pack[g] = packed(near_blocks[0, g].reshape(3 * points, points))


def near_kernel(
    near_list,
    coupling_list,
    charges,
    near_pack,
    coupling_pack,
    local_path,
    mine,
    from_inner,
    from_outer,
    known,
    window,
    sources,
):
    leaves = near_pack.shape[0]
    points = near_pack.shape[2] // 2
    rhs = charges.shape[1]
    levels = leaves.bit_length() - 1
    pairs = leaves - 1
    width = 2 * points
    reach = NEAR * points // width
    low_lanes = lax.broadcasted_iota(jnp.int32, (rhs, width), 1) < points

    def spread(pair, ref, even, odd):
        turned = pltpu.roll(pair, points, 1)
        ref[even] = jnp.where(low_lanes, pair, turned)
        ref[odd] = jnp.where(low_lanes, turned, pair)

    parity = lax.axis_index("leaf") & 1
    for k in range(reach):
        at = (1 - parity) * (NEAR + leaves) + 2 * k
        spread(from_inner[pairs + k], sources, at, at + 1)
        at = parity * (NEAR + leaves) + 2 * k
        spread(from_outer[pairs + k], sources, at, at + 1)
    for k in range(leaves // 2):
        at = NEAR + 2 * k
        spread(charges[0, :, k * width : (k + 1) * width], sources, at, at + 1)
    for height in range(levels):
        first, members = tier_span(leaves, height)
        for j in range(members // 2):
            k = first // 2 + j
            at = 3 * first + 2 * j
            spread(from_inner[k], window, at + (2 - 2 * parity) * members, at + (2 - 2 * parity) * members + 1)
            spread(mine[k], window, at + members, at + members + 1)
            spread(
                from_outer[k],
                window,
                at + 2 * parity * members,
                at + 2 * parity * members + 1,
            )

    def three(a, b, c):
        return beside(jnp.where(low_lanes, a, b), c[:, :points])

    def picked(ref, base, list_ref, n):
        return three(*(ref[base + list_ref[slot, 0, n]] for slot in range(3)))

    def product(left, weights):
        value = dot(stacked(left), weights)
        return value[:rhs] + jnp.where(low_lanes, value[rhs:], 0.0)

    def folded(value):
        return value + pltpu.roll(value, points, 1)

    coupled = []
    for n in range(2 * leaves - 2):
        height = next(h for h in range(levels) if n < sum(tier_span(leaves, h)))
        left = picked(window, 3 * tier_span(leaves, height)[0], coupling_list, n)
        coupled.append(folded(product(left, coupling_pack[n])))
    result = []
    for g in range(leaves):
        value = product(picked(sources, g, near_list, g), near_pack[g])
        chain = [coupled[tier_span(leaves, h)[0] + (g >> h)] for h in range(levels)]
        left = [
            jnp.where(low_lanes, chain[h], chain[h + 1]) if h + 1 < levels else chain[h][:, :points]
            for h in range(0, levels, 2)
        ]
        result.append(folded(value + product(jnp.concatenate(left, axis=1), local_path[g])))
    for j in range(leaves // 2):
        known[:, j * width : (j + 1) * width] = jnp.where(
            low_lanes, result[2 * j], result[2 * j + 1]
        )


def final_kernel(received, known, mats, path, coarse_transfer, out, *tier_refs):
    top_count, leaf_count = received.shape[0], received.shape[1]
    coarse = coarse_transfer.shape[1]
    rhs = out.shape[1]
    position = lax.axis_index("leaf")
    body = lax.axis_index("top")
    terms = []
    for s in range(top_count - 1):
        other = lax.rem(body + 1 + s, top_count)
        total = received[other, 0]
        for j in range(1, leaf_count):
            total = total + received[other, j]
        terms.append(unfold(total))

    def node(tier, index):
        if tier == 0:
            return unfold(received[body, index])
        return tier_refs[tier - 1][index]

    for tier in range(coarse - 2):
        count = leaf_count >> tier
        here = position >> tier
        odd = here & 1
        for offset in (-2, 2, jnp.where(odd == 1, -3, 3)):
            terms.append(node(tier, (here + offset + count) & (count - 1)))
        if tier < coarse - 3:
            for j in range(count // 2):
                tier_refs[tier][j] = mm(node(tier, 2 * j), coarse_transfer[0, tier, 0]) + mm(
                    node(tier, 2 * j + 1), coarse_transfer[0, tier, 1]
                )
    across = ((position >> (coarse - 2)) + 2) & 3
    terms.append(node(coarse - 3, 2 * across))
    terms.append(node(coarse - 3, 2 * across + 1))
    left = stacked(jnp.concatenate(terms, axis=1))
    value = dot(left, mats[0])
    left = stacked(value[:rhs] + value[rhs:] + dot(left[:rhs], mats[1]))
    value = dot(left, path[0])
    out[0] = known[...] + value[:rhs] + value[rhs:] + dot(left[:rhs], path[1])


def per_device(
    charges,
    leaf_basis,
    near_blocks,
    near_list,
    local_transfer,
    local_coupling,
    coupling_list,
    coarse_transfer,
    coarse_coupling,
    opposite_coupling,
    body_coupling,
):
    rhs = charges.shape[1]
    leaves, points, rank = leaf_basis.shape[1:]
    leaf_count = lax.axis_size("leaf")
    top_count = lax.axis_size("top")
    coarse = coarse_transfer.shape[1]
    packs = leaves - 1 + NEAR // 2
    f32 = jnp.float32
    vmem = pl.BlockSpec(memory_space=VMEM)
    smem = pl.BlockSpec(memory_space=SMEM)
    params = pltpu.CompilerParams(vmem_limit_bytes=8 << 20)
    pack_shape = jax.ShapeDtypeStruct((packs, rhs, 2 * rank), f32)
    hbm = pl.BlockSpec(memory_space=HBM)

    def like(*arrays):
        return tuple(jax.ShapeDtypeStruct(array.shape, array.dtype) for array in arrays)

    def stay(*arrays):
        return [pltpu.with_memory_space_constraint(array, HBM) for array in arrays]

    inner, outer, exchange, charges_v, basis_v, transfer_v, coarse_v, coupling_v = pl.pallas_call(
        up_kernel,
        out_shape=(
            pack_shape,
            pack_shape,
            jax.ShapeDtypeStruct((top_count, leaf_count, rhs // 2, 2 * rank), f32),
        )
        + like(charges, leaf_basis, local_transfer, coarse_transfer, local_coupling),
        in_specs=[hbm] * 5,
        out_specs=(vmem,) * 8,
        scratch_shapes=[pltpu.SemaphoreType.DMA((5,))],
        name="up",
        compiler_params=params,
        cost_estimate=pl.CostEstimate(flops=40_000_000, bytes_accessed=1_000_000, transcendentals=0),
    )(
        *stay(charges, leaf_basis, local_transfer, coarse_transfer, local_coupling)
    )
    inner_pairs = [(i, i ^ 1) for i in range(leaf_count)]
    outer_pairs = [(i, (i + (1 if i & 1 else -1)) % leaf_count) for i in range(leaf_count)]
    from_inner = lax.ppermute(inner, "leaf", inner_pairs)
    from_outer = lax.ppermute(outer, "leaf", outer_pairs)
    received = lax.all_to_all(
        exchange.reshape(leaf_count * top_count, rhs // 2, 2 * rank),
        ("top", "leaf"),
        0,
        0,
        tiled=True,
    ).reshape(exchange.shape)
    terms = (top_count - 1) + 3 * (coarse - 2) + 2
    levels = leaves.bit_length() - 1
    bf16 = jnp.bfloat16
    mats, path, local_path, near_pack, coupling_pack = pl.pallas_call(
        prep_kernel,
        out_shape=(
            jax.ShapeDtypeStruct((2, terms * rank, rank), bf16),
            jax.ShapeDtypeStruct((2, rank, leaves * points), bf16),
            jax.ShapeDtypeStruct((leaves, levels * rank, 2 * points), bf16),
            jax.ShapeDtypeStruct((leaves, 3 * points, 2 * points), bf16),
            jax.ShapeDtypeStruct((2 * leaves - 2, 3 * rank, 2 * rank), bf16),
        ),
        in_specs=[vmem] * 4 + [hbm] * 4,
        out_specs=(vmem,) * 5,
        scratch_shapes=[
            pltpu.VMEM(array.shape, f32)
            for array in (coarse_coupling, opposite_coupling, body_coupling, near_blocks)
        ]
        + [pltpu.SemaphoreType.DMA((4,))],
        name="prep",
        compiler_params=params,
        cost_estimate=pl.CostEstimate(flops=40_000_000, bytes_accessed=2_000_000, transcendentals=0),
    )(
        basis_v,
        transfer_v,
        coarse_v,
        coupling_v,
        *stay(coarse_coupling, opposite_coupling, body_coupling, near_blocks),
    )
    known = pl.pallas_call(
        near_kernel,
        out_shape=jax.ShapeDtypeStruct((rhs, leaves * points), f32),
        in_specs=[smem] * 2 + [vmem] * 7,
        out_specs=vmem,
        scratch_shapes=[
            pltpu.VMEM((3 * (2 * leaves - 2), rhs, 2 * rank), f32),
            pltpu.VMEM((leaves + 2 * NEAR, rhs, 2 * points), f32),
        ],
        name="near",
        compiler_params=params,
        cost_estimate=pl.CostEstimate(flops=80_000_000, bytes_accessed=3_000_000, transcendentals=0),
    )(
        jnp.transpose(near_list, (2, 0, 1)),
        jnp.transpose(coupling_list, (2, 0, 1)),
        charges_v,
        near_pack,
        coupling_pack,
        local_path,
        inner,
        from_inner,
        from_outer,
    )
    return pl.pallas_call(
        final_kernel,
        out_shape=jax.ShapeDtypeStruct(charges.shape, f32),
        in_specs=[vmem] * 5,
        out_specs=vmem,
        scratch_shapes=[
            pltpu.VMEM((leaf_count >> (tier + 1), rhs, rank), f32) for tier in range(coarse - 3)
        ],
        name="final",
        compiler_params=params,
        cost_estimate=pl.CostEstimate(flops=10_000_000, bytes_accessed=600_000, transcendentals=0),
    )(received, known, mats, path, coarse_v)


def solution(mesh):
    in_specs = (
        P("top", None, "leaf"),
        P("top", "leaf", None, None),
        P("top", "leaf", None, None, None),
        P("top", "leaf", None),
        P("top", "leaf", None, None),
        P("top", "leaf", None, None, None),
        P("top", "leaf", None),
        P("top", None, None, None, None),
        P("top", None, None, None, None),
        P("top", None, None),
        P("top", None, None, None),
    )
    out_specs = P("top", None, "leaf")
    return jax.shard_map(
        per_device, mesh=mesh, in_specs=in_specs, out_specs=out_specs, check_vma=False
    )
```

```python
import jax
import jax.numpy as jnp
from jax import lax
from jax.experimental import pallas as pl
from jax.experimental.pallas import tpu as pltpu
from jax.sharding import PartitionSpec as P

NEAR = 4
HIGH = lax.Precision.HIGH
VMEM = pltpu.MemorySpace.VMEM
SMEM = pltpu.MemorySpace.SMEM
HBM = pltpu.MemorySpace.HBM


def mm(a, b):
    return lax.dot_general(
        a, b, (((1,), (0,)), ((), ())), precision=HIGH, preferred_element_type=jnp.float32
    )


def mm_t(a, b):
    return lax.dot_general(
        a, b, (((1,), (1,)), ((), ())), precision=HIGH, preferred_element_type=jnp.float32
    )


def halves(x):
    high = x.astype(jnp.bfloat16)
    return high, (x - high.astype(jnp.float32)).astype(jnp.bfloat16)


def packed(x):
    high = x.astype(jnp.bfloat16).astype(jnp.float32)
    return beside(high, x - high).astype(jnp.bfloat16)


def stacked(x):
    high, low = halves(x)
    return jnp.concatenate([high, low], axis=0)


def mm_s(a, b):
    rows = a.shape[0]
    left = stacked(a)
    high, low = halves(b)
    value = dot(left, high)
    return value[:rhs_of(value)] + value[rhs_of(value):] + dot(left[:rows], low)


def rhs_of(value):
    return value.shape[0] // 2


def dot(a, b):
    return lax.dot_general(a, b, (((1,), (0,)), ((), ())), preferred_element_type=jnp.float32)


def beside(a, b):
    return jnp.concatenate([a, b], axis=1)


def fold(x):
    half = x.shape[0] // 2
    return beside(x[:half], x[half:])


def unfold(x):
    half = x.shape[1] // 2
    return jnp.concatenate([x[:, :half], x[:, half:]], axis=0)


def tier_span(leaves, height):
    members = leaves >> height
    return 2 * leaves - 2 * members, members


def path_product(coarse_ref, position, tiers):
    product = None
    products = []
    for tier in range(tiers):
        matrix = coarse_ref[0, tier, (position >> tier) & 1]
        product = matrix if product is None else mm(product, matrix)
        products.append(product)
    return products


def fetch(sources, targets, sem):
    copies = [
        pltpu.make_async_copy(source, target, sem.at[i])
        for i, (source, target) in enumerate(zip(sources, targets))
    ]
    for copy in copies:
        copy.start()
    return copies


def up_kernel(
    charges_hbm,
    basis_hbm,
    transfer_hbm,
    coarse_hbm,
    coupling_hbm,
    ahead,
    behind,
    exchange,
    charges,
    basis,
    transfer,
    coarse_transfer,
    coupling,
    sem,
):
    copies = fetch(
        (charges_hbm, basis_hbm, coarse_hbm, transfer_hbm, coupling_hbm),
        (charges, basis, coarse_transfer, transfer, coupling),
        sem,
    )
    leaves, points = basis.shape[1], basis.shape[2]
    levels = leaves.bit_length() - 1
    position = lax.axis_index("leaf")
    body = lax.axis_index("top")
    top_count = exchange.shape[0]
    width = 2 * points
    reach = NEAR * points // width
    whole = leaves // 2
    pairs = leaves - 1
    copies[0].wait()
    copies[1].wait()
    for k in range(reach):
        first = (whole - reach + k) * width
        high = charges[0, :, first : first + width]
        low = charges[0, :, k * width : (k + 1) * width]
        ahead[pairs + k] = high
        behind[pairs + k] = low
    coeffs = [mm_s(charges[0, :, g * points : (g + 1) * points], basis[0, g]) for g in range(leaves)]
    copies[2].wait()
    copies[3].wait()
    tiers = coarse_transfer.shape[1]
    first, members = tier_span(leaves, levels - 1)
    steps = [coarse_transfer[0, tier, (position >> tier) & 1] for tier in range(tiers)]
    ends = [mm(transfer[0, first + n], steps[0]) for n in range(members)]
    rest = None
    for step in steps[:0:-1]:
        rest = step if rest is None else mm(step, rest)
    ends = [mm(end, rest) for end in ends]
    for height in range(levels):
        first, members = tier_span(leaves, height)
        for j in range(members // 2):
            pair = beside(coeffs[2 * j], coeffs[2 * j + 1])
            ahead[first // 2 + j] = pair
            behind[first // 2 + j] = pair
        below = coeffs
        coeffs = [
            mm_s(below[2 * j], transfer[0, first + 2 * j])
            + mm_s(below[2 * j + 1], transfer[0, first + 2 * j + 1])
            for j in range(members // 2)
        ]
    own = fold(coeffs[0])
    other = fold(mm_s(below[0], ends[0]) + mm_s(below[1], ends[1]))
    for t in range(top_count):
        value = jnp.where(body == t, own, other)
        exchange[t] = jnp.broadcast_to(value[None], (exchange.shape[1],) + value.shape)
    copies[4].wait()


def paths(basis, transfer, path, leaf_path, pair_path):
    leaves, points, rank = basis.shape[1:]
    levels = leaves.bit_length() - 1
    flipped = [basis[0, g].T for g in range(leaves)]
    for g in range(leaves):
        leaf_path[g] = packed(flipped[g])
    wide = [
        beside(*(mm_s(transfer[0, g].T, flipped[g]) for g in (2 * j, 2 * j + 1)))
        for j in range(leaves // 2)
    ]
    width = 2 * points
    for height in range(1, levels):
        first, members = tier_span(leaves, height)
        for j in range(leaves // 2):
            group = leaves // 2 // len(wide)
            at = (j % group) * width
            rows = slice((height - 1) * rank, height * rank)
            pair_path[j, rows, :width], pair_path[j, rows, width:] = halves(
                wide[j // group][:, at : at + width]
            )
        if len(wide) > members:
            wide = [beside(wide[2 * n], wide[2 * n + 1]) for n in range(members)]
        wide = [mm_s(transfer[0, first + n].T, wide[n]) for n in range(members)]
    for n in range(len(wide)):
        size = leaves * points // len(wide)
        columns = slice(n * size, (n + 1) * size)
        path[0, :, columns], path[1, :, columns] = halves(wide[n])


def prep_kernel(
    basis,
    transfer,
    coarse_transfer,
    coupling,
    coarse_coupling_hbm,
    opposite_hbm,
    body_coupling_hbm,
    near_hbm,
    path,
    leaf_path,
    pair_path,
    mats,
    near_pack,
    coupling_pack,
    coarse_coupling,
    opposite,
    body_coupling,
    near_blocks,
    sem,
):
    copies = fetch(
        (coarse_coupling_hbm, opposite_hbm, body_coupling_hbm, near_hbm),
        (coarse_coupling, opposite, body_coupling, near_blocks),
        sem,
    )
    position = lax.axis_index("leaf")


    @pl.when(position >= 0)
    def _():
        paths(basis, transfer, path, leaf_path, pair_path)

    leaves, points, rank = basis.shape[1:]
    coarse = coarse_transfer.shape[1]
    for n in range(2 * leaves - 2):
        coupling_pack[n] = packed(coupling[0, n].reshape(3 * rank, rank))
    products = path_product(coarse_transfer, position, coarse)
    at = 0

    def put(value):
        nonlocal at
        rows = slice(at, at + rank)
        mats[0, rows], mats[1, rows] = halves(value)
        at += rank

    for copy in copies[:3]:
        copy.wait()
    for s in range(body_coupling.shape[1]):
        put(mm_t(body_coupling[0, s], products[coarse - 1]))
    for tier in range(coarse - 2):
        odd = (position >> tier) & 1
        for slot in (1, 2, jnp.where(odd == 1, 0, 3)):
            value = coarse_coupling[0, tier, slot]
            put(value if tier == 0 else mm_t(value, products[tier - 1]))
    far = mm_t(opposite[0], products[coarse - 3])
    put(mm(coarse_transfer[0, coarse - 3, 0], far))
    put(mm(coarse_transfer[0, coarse - 3, 1], far))
    copies[3].wait()
    for g in range(leaves):
        near_pack[g] = packed(near_blocks[0, g].reshape(3 * points, points))


def near_kernel(
    near_list,
    coupling_list,
    charges,
    near_pack,
    coupling_pack,
    leaf_path,
    pair_path,
    mine,
    below,
    above,
    known,
    window,
    sources,
):
    leaves = near_pack.shape[0]
    points = near_pack.shape[2] // 2
    rhs = charges.shape[1]
    levels = leaves.bit_length() - 1
    pairs = leaves - 1
    width = 2 * points
    reach = NEAR * points // width
    low_lanes = lax.broadcasted_iota(jnp.int32, (rhs, width), 1) < points

    def spread(pair, ref, even, odd):
        turned = pltpu.roll(pair, points, 1)
        ref[even] = jnp.where(low_lanes, pair, turned)
        ref[odd] = jnp.where(low_lanes, turned, pair)

    for k in range(reach):
        spread(below[pairs + k], sources, 2 * k, 2 * k + 1)
        at = NEAR + leaves + 2 * k
        spread(above[pairs + k], sources, at, at + 1)
    for k in range(leaves // 2):
        at = NEAR + 2 * k
        spread(charges[0, :, k * width : (k + 1) * width], sources, at, at + 1)
    for height in range(levels):
        first, members = tier_span(leaves, height)
        for block, pack in enumerate((below, mine, above)):
            for j in range(members // 2):
                at = 3 * first + block * members + 2 * j
                spread(pack[first // 2 + j], window, at, at + 1)

    def three(a, b, c):
        return beside(jnp.where(low_lanes, a, b), c[:, :points])

    def picked(ref, base, list_ref, n):
        return three(*(ref[base + list_ref[slot, 0, n]] for slot in range(3)))

    def product(left, weights):
        value = dot(stacked(left), weights)
        return value[:rhs] + jnp.where(low_lanes, value[rhs:], 0.0)

    def folded(value):
        return value + pltpu.roll(value, points, 1)

    coupled = []
    for n in range(2 * leaves - 2):
        height = next(h for h in range(levels) if n < sum(tier_span(leaves, h)))
        left = picked(window, 3 * tier_span(leaves, height)[0], coupling_list, n)
        coupled.append(folded(product(left, coupling_pack[n])))
    result = []
    for g in range(leaves):
        value = product(picked(sources, g, near_list, g), near_pack[g])
        result.append(folded(value + product(coupled[g][:, :points], leaf_path[g])))
    for j in range(leaves // 2):
        chain = [coupled[tier_span(leaves, h)[0] + (2 * j >> h)] for h in range(1, levels)]
        left = [
            jnp.where(low_lanes, *chain[h : h + 2]) if h + 1 < len(chain) else chain[h][:, :points]
            for h in range(0, len(chain), 2)
        ]
        value = dot(stacked(jnp.concatenate(left, axis=1)), pair_path[j])
        value = value[:rhs, :width] + value[:rhs, width:] + value[rhs:, :width]
        known[:, j * width : (j + 1) * width] = value + jnp.where(
            low_lanes, result[2 * j], result[2 * j + 1]
        )


def final_kernel(received, known, mats, path, coarse_transfer, out, *tier_refs):
    top_count, leaf_count = received.shape[0], received.shape[1]
    coarse = coarse_transfer.shape[1]
    rhs = out.shape[1]
    position = lax.axis_index("leaf")
    body = lax.axis_index("top")
    terms = []
    for s in range(top_count - 1):
        other = lax.rem(body + 1 + s, top_count)
        total = received[other, 0]
        for j in range(1, leaf_count):
            total = total + received[other, j]
        terms.append(unfold(total))

    def node(tier, index):
        if tier == 0:
            return unfold(received[body, index])
        return tier_refs[tier - 1][index]

    for tier in range(coarse - 2):
        count = leaf_count >> tier
        here = position >> tier
        odd = here & 1
        for offset in (-2, 2, jnp.where(odd == 1, -3, 3)):
            terms.append(node(tier, (here + offset + count) & (count - 1)))
        if tier < coarse - 3:
            for j in range(count // 2):
                tier_refs[tier][j] = mm(node(tier, 2 * j), coarse_transfer[0, tier, 0]) + mm(
                    node(tier, 2 * j + 1), coarse_transfer[0, tier, 1]
                )
    across = ((position >> (coarse - 2)) + 2) & 3
    terms.append(node(coarse - 3, 2 * across))
    terms.append(node(coarse - 3, 2 * across + 1))
    left = stacked(jnp.concatenate(terms, axis=1))
    value = dot(left, mats[0])
    left = stacked(value[:rhs] + value[rhs:] + dot(left[:rhs], mats[1]))
    value = dot(left, path[0])
    out[0] = known[...] + value[:rhs] + value[rhs:] + dot(left[:rhs], path[1])


def per_device(
    charges,
    leaf_basis,
    near_blocks,
    near_list,
    local_transfer,
    local_coupling,
    coupling_list,
    coarse_transfer,
    coarse_coupling,
    opposite_coupling,
    body_coupling,
):
    rhs = charges.shape[1]
    leaves, points, rank = leaf_basis.shape[1:]
    leaf_count = lax.axis_size("leaf")
    top_count = lax.axis_size("top")
    coarse = coarse_transfer.shape[1]
    packs = leaves - 1 + NEAR // 2
    f32 = jnp.float32
    vmem = pl.BlockSpec(memory_space=VMEM)
    smem = pl.BlockSpec(memory_space=SMEM)
    params = pltpu.CompilerParams(vmem_limit_bytes=8 << 20)
    pack_shape = jax.ShapeDtypeStruct((packs, rhs, 2 * rank), f32)
    hbm = pl.BlockSpec(memory_space=HBM)

    def like(*arrays):
        return tuple(jax.ShapeDtypeStruct(array.shape, array.dtype) for array in arrays)

    def stay(*arrays):
        return [pltpu.with_memory_space_constraint(array, HBM) for array in arrays]

    ahead, behind, exchange, charges_v, basis_v, transfer_v, coarse_v, coupling_v = pl.pallas_call(
        up_kernel,
        out_shape=(
            pack_shape,
            pack_shape,
            jax.ShapeDtypeStruct((top_count, leaf_count, rhs // 2, 2 * rank), f32),
        )
        + like(charges, leaf_basis, local_transfer, coarse_transfer, local_coupling),
        in_specs=[hbm] * 5,
        out_specs=(vmem,) * 8,
        scratch_shapes=[pltpu.SemaphoreType.DMA((5,))],
        name="up",
        compiler_params=params,
        cost_estimate=pl.CostEstimate(flops=40_000_000, bytes_accessed=1_000_000, transcendentals=0),
    )(
        *stay(charges, leaf_basis, local_transfer, coarse_transfer, local_coupling)
    )
    forward = [(i, (i + 1) % leaf_count) for i in range(leaf_count)]
    backward = [(target, source) for source, target in forward]
    below = lax.ppermute(ahead, "leaf", forward)
    above = lax.ppermute(behind, "leaf", backward)
    received = lax.all_to_all(
        exchange.reshape(leaf_count * top_count, rhs // 2, 2 * rank),
        ("top", "leaf"),
        0,
        0,
        tiled=True,
    ).reshape(exchange.shape)
    terms = (top_count - 1) + 3 * (coarse - 2) + 2
    levels = leaves.bit_length() - 1
    bf16 = jnp.bfloat16
    path, leaf_path, pair_path, mats, near_pack, coupling_pack = pl.pallas_call(
        prep_kernel,
        out_shape=(
            jax.ShapeDtypeStruct((2, rank, leaves * points), bf16),
            jax.ShapeDtypeStruct((leaves, rank, 2 * points), bf16),
            jax.ShapeDtypeStruct((leaves // 2, (levels - 1) * rank, 4 * points), bf16),
            jax.ShapeDtypeStruct((2, terms * rank, rank), bf16),
            jax.ShapeDtypeStruct((leaves, 3 * points, 2 * points), bf16),
            jax.ShapeDtypeStruct((2 * leaves - 2, 3 * rank, 2 * rank), bf16),
        ),
        in_specs=[vmem] * 4 + [hbm] * 4,
        out_specs=(vmem,) * 6,
        scratch_shapes=[
            pltpu.VMEM(array.shape, f32)
            for array in (coarse_coupling, opposite_coupling, body_coupling, near_blocks)
        ]
        + [pltpu.SemaphoreType.DMA((4,))],
        name="prep",
        compiler_params=params,
        cost_estimate=pl.CostEstimate(flops=20_000_000, bytes_accessed=2_000_000, transcendentals=0),
    )(
        basis_v,
        transfer_v,
        coarse_v,
        coupling_v,
        *stay(coarse_coupling, opposite_coupling, body_coupling, near_blocks),
    )
    known = pl.pallas_call(
        near_kernel,
        out_shape=jax.ShapeDtypeStruct((rhs, leaves * points), f32),
        in_specs=[smem] * 2 + [vmem] * 8,
        out_specs=vmem,
        scratch_shapes=[
            pltpu.VMEM((3 * (2 * leaves - 2), rhs, 2 * rank), f32),
            pltpu.VMEM((leaves + 2 * NEAR, rhs, 2 * points), f32),
        ],
        name="near",
        compiler_params=params,
        cost_estimate=pl.CostEstimate(flops=80_000_000, bytes_accessed=3_000_000, transcendentals=0),
    )(
        jnp.transpose(near_list, (2, 0, 1)),
        jnp.transpose(coupling_list, (2, 0, 1)),
        charges_v,
        near_pack,
        coupling_pack,
        leaf_path,
        pair_path,
        ahead,
        below,
        above,
    )
    return pl.pallas_call(
        final_kernel,
        out_shape=jax.ShapeDtypeStruct(charges.shape, f32),
        in_specs=[vmem] * 5,
        out_specs=vmem,
        scratch_shapes=[
            pltpu.VMEM((leaf_count >> (tier + 1), rhs, rank), f32) for tier in range(coarse - 3)
        ],
        name="final",
        compiler_params=params,
        cost_estimate=pl.CostEstimate(flops=10_000_000, bytes_accessed=600_000, transcendentals=0),
    )(received, known, mats, path, coarse_v)


def solution(mesh):
    in_specs = (
        P("top", None, "leaf"),
        P("top", "leaf", None, None),
        P("top", "leaf", None, None, None),
        P("top", "leaf", None),
        P("top", "leaf", None, None),
        P("top", "leaf", None, None, None),
        P("top", "leaf", None),
        P("top", None, None, None, None),
        P("top", None, None, None, None),
        P("top", None, None),
        P("top", None, None, None),
    )
    out_specs = P("top", None, "leaf")
    return jax.shard_map(
        per_device, mesh=mesh, in_specs=in_specs, out_specs=out_specs, check_vma=False
    )
```

```python
import jax
import jax.numpy as jnp
from jax import lax
from jax.experimental import pallas as pl
from jax.experimental.pallas import tpu as pltpu
from jax.sharding import PartitionSpec as P

NEAR = 4
HIGH = lax.Precision.HIGH
VMEM = pltpu.MemorySpace.VMEM
SMEM = pltpu.MemorySpace.SMEM
HBM = pltpu.MemorySpace.HBM


def mm(a, b):
    return lax.dot_general(
        a, b, (((1,), (0,)), ((), ())), precision=HIGH, preferred_element_type=jnp.float32
    )


def mm_t(a, b):
    return lax.dot_general(
        a, b, (((1,), (1,)), ((), ())), precision=HIGH, preferred_element_type=jnp.float32
    )


def halves(x):
    high = x.astype(jnp.bfloat16)
    return high, (x - high.astype(jnp.float32)).astype(jnp.bfloat16)


def packed(x):
    high = x.astype(jnp.bfloat16).astype(jnp.float32)
    return beside(high, x - high).astype(jnp.bfloat16)


def stacked(x):
    high, low = halves(x)
    return jnp.concatenate([high, low], axis=0)


def mm_s(a, b):
    rows = a.shape[0]
    left = stacked(a)
    high, low = halves(b)
    value = dot(left, high)
    return value[:rhs_of(value)] + value[rhs_of(value):] + dot(left[:rows], low)


def rhs_of(value):
    return value.shape[0] // 2


def dot(a, b):
    return lax.dot_general(a, b, (((1,), (0,)), ((), ())), preferred_element_type=jnp.float32)


def beside(a, b):
    return jnp.concatenate([a, b], axis=1)


def unfold(x):
    half = x.shape[1] // 2
    return jnp.concatenate([x[:, :half], x[:, half:]], axis=0)


def tier_span(leaves, height):
    members = leaves >> height
    return 2 * leaves - 2 * members, members


def path_product(coarse_ref, position, tiers):
    product = None
    products = []
    for tier in range(tiers):
        matrix = coarse_ref[0, tier, (position >> tier) & 1]
        product = matrix if product is None else mm(product, matrix)
        products.append(product)
    return products


def fetch(sources, targets, sem):
    copies = [
        pltpu.make_async_copy(source, target, sem.at[i])
        for i, (source, target) in enumerate(zip(sources, targets))
    ]
    for copy in copies:
        copy.start()
    return copies


def up_kernel(
    charges_hbm,
    basis_hbm,
    transfer_hbm,
    coarse_hbm,
    coupling_hbm,
    ahead,
    behind,
    exchange,
    charges,
    basis,
    transfer,
    coarse_transfer,
    coupling,
    sem,
):
    copies = fetch(
        (charges_hbm, basis_hbm, coarse_hbm, transfer_hbm, coupling_hbm),
        (charges, basis, coarse_transfer, transfer, coupling),
        sem,
    )
    leaves, points = basis.shape[1], basis.shape[2]
    levels = leaves.bit_length() - 1
    position = lax.axis_index("leaf")
    body = lax.axis_index("top")
    top_count = exchange.shape[0]
    width = 2 * points
    reach = NEAR * points // width
    whole = leaves // 2
    pairs = leaves - 1
    copies[0].wait()
    copies[1].wait()
    for k in range(reach):
        first = (whole - reach + k) * width
        high = charges[0, :, first : first + width]
        low = charges[0, :, k * width : (k + 1) * width]
        ahead[pairs + k] = high
        behind[pairs + k] = low
    rhs = charges.shape[1]
    low_lanes = lax.broadcasted_iota(jnp.int32, (rhs, width), 1) < points
    coeffs = []
    for j in range(whole):
        pair = charges[0, :, j * width : (j + 1) * width]
        left = jnp.concatenate(
            [jnp.where(low_lanes, pair, 0.0), jnp.where(low_lanes, 0.0, pair)], axis=0
        )
        value = mm_s(left, basis[0, 2 * j : 2 * j + 2].reshape(width, basis.shape[3]))
        coeffs += [value[:rhs], value[rhs:]]
    copies[2].wait()
    copies[3].wait()
    tiers = coarse_transfer.shape[1]
    first, members = tier_span(leaves, levels - 1)
    steps = [coarse_transfer[0, tier, (position >> tier) & 1] for tier in range(tiers)]
    ends = [mm_s(transfer[0, first + n], steps[0]) for n in range(members)]
    rest = beside(steps[-1], steps[-1])
    for step in steps[-2:0:-1]:
        rest = mm_s(step, rest)
    ends = [mm_s(end, rest) for end in ends]
    tops = [beside(transfer[0, first + n], transfer[0, first + n]) for n in range(members)]
    for height in range(levels):
        first, members = tier_span(leaves, height)
        for j in range(members // 2):
            pair = beside(coeffs[2 * j], coeffs[2 * j + 1])
            ahead[first // 2 + j] = pair
            behind[first // 2 + j] = pair
        if height < levels - 1:
            coeffs = [
                mm_s(coeffs[2 * j], transfer[0, first + 2 * j])
                + mm_s(coeffs[2 * j + 1], transfer[0, first + 2 * j + 1])
                for j in range(members // 2)
            ]
    half = rhs // 2

    def doubled(weights):
        value = mm_s(coeffs[0], weights[0]) + mm_s(coeffs[1], weights[1])
        return jnp.where(low_lanes[:half], value[:half], value[half:])

    own = doubled(tops)
    other = doubled(ends)
    for t in range(top_count):
        value = jnp.where(body == t, own, other)
        exchange[t] = jnp.broadcast_to(value[None], (exchange.shape[1],) + value.shape)
    copies[4].wait()


def paths(basis, transfer, path, leaf_path, pair_path):
    leaves, points, rank = basis.shape[1:]
    levels = leaves.bit_length() - 1
    flipped = [basis[0, g].T for g in range(leaves)]
    for g in range(leaves):
        leaf_path[g] = packed(flipped[g])
    wide = [
        beside(*(mm_s(transfer[0, g].T, flipped[g]) for g in (2 * j, 2 * j + 1)))
        for j in range(leaves // 2)
    ]
    width = 2 * points
    for height in range(1, levels):
        first, members = tier_span(leaves, height)
        for j in range(leaves // 2):
            group = leaves // 2 // len(wide)
            at = (j % group) * width
            rows = slice((height - 1) * rank, height * rank)
            pair_path[j, rows, :width], pair_path[j, rows, width:] = halves(
                wide[j // group][:, at : at + width]
            )
        if len(wide) > members:
            wide = [beside(wide[2 * n], wide[2 * n + 1]) for n in range(members)]
        wide = [mm_s(transfer[0, first + n].T, wide[n]) for n in range(members)]
    for n in range(len(wide)):
        size = leaves * points // len(wide)
        columns = slice(n * size, (n + 1) * size)
        path[0, :, columns], path[1, :, columns] = halves(wide[n])


def prep_kernel(
    basis,
    transfer,
    coarse_transfer,
    coupling,
    coarse_coupling_hbm,
    opposite_hbm,
    body_coupling_hbm,
    near_hbm,
    path,
    leaf_path,
    pair_path,
    mats,
    near_pack,
    coupling_pack,
    coarse_coupling,
    opposite,
    body_coupling,
    near_blocks,
    sem,
):
    copies = fetch(
        (coarse_coupling_hbm, opposite_hbm, body_coupling_hbm, near_hbm),
        (coarse_coupling, opposite, body_coupling, near_blocks),
        sem,
    )
    position = lax.axis_index("leaf")


    @pl.when(position >= 0)
    def _():
        paths(basis, transfer, path, leaf_path, pair_path)

    leaves, points, rank = basis.shape[1:]
    coarse = coarse_transfer.shape[1]
    for n in range(2 * leaves - 2):
        coupling_pack[n] = packed(coupling[0, n].reshape(3 * rank, rank))
    products = path_product(coarse_transfer, position, coarse)
    at = 0

    def put(value):
        nonlocal at
        rows = slice(at, at + rank)
        mats[0, rows], mats[1, rows] = halves(value)
        at += rank

    for copy in copies[:3]:
        copy.wait()
    for s in range(body_coupling.shape[1]):
        put(mm_t(body_coupling[0, s], products[coarse - 1]))
    for tier in range(coarse - 2):
        odd = (position >> tier) & 1
        for slot in (1, 2, jnp.where(odd == 1, 0, 3)):
            value = coarse_coupling[0, tier, slot]
            put(value if tier == 0 else mm_t(value, products[tier - 1]))
    far = mm_t(opposite[0], products[coarse - 3])
    put(mm(coarse_transfer[0, coarse - 3, 0], far))
    put(mm(coarse_transfer[0, coarse - 3, 1], far))
    copies[3].wait()
    for g in range(leaves):
        near_pack[g] = packed(near_blocks[0, g].reshape(3 * points, points))


def near_kernel(
    near_list,
    coupling_list,
    charges,
    near_pack,
    coupling_pack,
    leaf_path,
    pair_path,
    mine,
    below,
    above,
    known,
    window,
    sources,
):
    leaves = near_pack.shape[0]
    points = near_pack.shape[2] // 2
    rhs = charges.shape[1]
    levels = leaves.bit_length() - 1
    pairs = leaves - 1
    width = 2 * points
    reach = NEAR * points // width
    low_lanes = lax.broadcasted_iota(jnp.int32, (rhs, width), 1) < points

    def spread(pair, ref, even, odd):
        turned = pltpu.roll(pair, points, 1)
        ref[even] = jnp.where(low_lanes, pair, turned)
        ref[odd] = jnp.where(low_lanes, turned, pair)

    for k in range(reach):
        spread(below[pairs + k], sources, 2 * k, 2 * k + 1)
        at = NEAR + leaves + 2 * k
        spread(above[pairs + k], sources, at, at + 1)
    for k in range(leaves // 2):
        at = NEAR + 2 * k
        spread(charges[0, :, k * width : (k + 1) * width], sources, at, at + 1)
    for height in range(levels):
        first, members = tier_span(leaves, height)
        for block, pack in enumerate((below, mine, above)):
            for j in range(members // 2):
                at = 3 * first + block * members + 2 * j
                spread(pack[first // 2 + j], window, at, at + 1)

    def three(a, b, c):
        return beside(jnp.where(low_lanes, a, b), c[:, :points])

    def picked(ref, base, list_ref, n):
        return three(*(ref[base + list_ref[slot, 0, n]] for slot in range(3)))

    def product(left, weights):
        value = dot(stacked(left), weights)
        return value[:rhs] + jnp.where(low_lanes, value[rhs:], 0.0)

    def folded(value):
        return value + pltpu.roll(value, points, 1)

    coupled = []
    for n in range(2 * leaves - 2):
        height = next(h for h in range(levels) if n < sum(tier_span(leaves, h)))
        left = picked(window, 3 * tier_span(leaves, height)[0], coupling_list, n)
        coupled.append(folded(product(left, coupling_pack[n])))
    result = []
    for g in range(leaves):
        value = product(picked(sources, g, near_list, g), near_pack[g])
        result.append(value + product(coupled[g][:, :points], leaf_path[g]))
    for j in range(leaves // 2):
        chain = [coupled[tier_span(leaves, h)[0] + (2 * j >> h)] for h in range(1, levels)]
        left = [
            jnp.where(low_lanes, *chain[h : h + 2]) if h + 1 < len(chain) else chain[h][:, :points]
            for h in range(0, len(chain), 2)
        ]
        value = dot(stacked(jnp.concatenate(left, axis=1)), pair_path[j])
        value = value[:rhs, :width] + value[:rhs, width:] + value[rhs:, :width]
        even, odd = result[2 * j], result[2 * j + 1]
        value = value + jnp.where(low_lanes, even, odd)
        known[:, j * width : (j + 1) * width] = value + pltpu.roll(
            jnp.where(low_lanes, odd, even), points, 1
        )


def final_kernel(received, known, mats, path, coarse_transfer, out, *tier_refs):
    top_count, leaf_count = received.shape[0], received.shape[1]
    coarse = coarse_transfer.shape[1]
    rhs = out.shape[1]
    position = lax.axis_index("leaf")
    body = lax.axis_index("top")
    terms = []
    for s in range(top_count - 1):
        other = lax.rem(body + 1 + s, top_count)
        total = received[other, 0]
        for j in range(1, leaf_count):
            total = total + received[other, j]
        terms.append(unfold(total))

    def node(tier, index):
        if tier == 0:
            return unfold(received[body, index])
        return tier_refs[tier - 1][index]

    for tier in range(coarse - 2):
        count = leaf_count >> tier
        here = position >> tier
        odd = here & 1
        for offset in (-2, 2, jnp.where(odd == 1, -3, 3)):
            terms.append(node(tier, (here + offset + count) & (count - 1)))
        if tier < coarse - 3:
            for j in range(count // 2):
                tier_refs[tier][j] = mm(node(tier, 2 * j), coarse_transfer[0, tier, 0]) + mm(
                    node(tier, 2 * j + 1), coarse_transfer[0, tier, 1]
                )
    across = ((position >> (coarse - 2)) + 2) & 3
    terms.append(node(coarse - 3, 2 * across))
    terms.append(node(coarse - 3, 2 * across + 1))
    left = stacked(jnp.concatenate(terms, axis=1))
    value = dot(left, mats[0])
    left = stacked(value[:rhs] + value[rhs:] + dot(left[:rhs], mats[1]))
    value = dot(left, path[0])
    out[0] = known[...] + value[:rhs] + value[rhs:] + dot(left[:rhs], path[1])


def per_device(
    charges,
    leaf_basis,
    near_blocks,
    near_list,
    local_transfer,
    local_coupling,
    coupling_list,
    coarse_transfer,
    coarse_coupling,
    opposite_coupling,
    body_coupling,
):
    rhs = charges.shape[1]
    leaves, points, rank = leaf_basis.shape[1:]
    leaf_count = lax.axis_size("leaf")
    top_count = lax.axis_size("top")
    coarse = coarse_transfer.shape[1]
    packs = leaves - 1 + NEAR // 2
    f32 = jnp.float32
    vmem = pl.BlockSpec(memory_space=VMEM)
    smem = pl.BlockSpec(memory_space=SMEM)
    params = pltpu.CompilerParams(vmem_limit_bytes=8 << 20)
    pack_shape = jax.ShapeDtypeStruct((packs, rhs, 2 * rank), f32)
    hbm = pl.BlockSpec(memory_space=HBM)

    def like(*arrays):
        return tuple(jax.ShapeDtypeStruct(array.shape, array.dtype) for array in arrays)

    def stay(*arrays):
        return [pltpu.with_memory_space_constraint(array, HBM) for array in arrays]

    ahead, behind, exchange, charges_v, basis_v, transfer_v, coarse_v, coupling_v = pl.pallas_call(
        up_kernel,
        out_shape=(
            pack_shape,
            pack_shape,
            jax.ShapeDtypeStruct((top_count, leaf_count, rhs // 2, 2 * rank), f32),
        )
        + like(charges, leaf_basis, local_transfer, coarse_transfer, local_coupling),
        in_specs=[hbm] * 5,
        out_specs=(vmem,) * 8,
        scratch_shapes=[pltpu.SemaphoreType.DMA((5,))],
        name="up",
        compiler_params=params,
        cost_estimate=pl.CostEstimate(flops=40_000_000, bytes_accessed=1_000_000, transcendentals=0),
    )(
        *stay(charges, leaf_basis, local_transfer, coarse_transfer, local_coupling)
    )
    forward = [(i, (i + 1) % leaf_count) for i in range(leaf_count)]
    backward = [(target, source) for source, target in forward]
    below = lax.ppermute(ahead, "leaf", forward)
    above = lax.ppermute(behind, "leaf", backward)
    received = lax.all_to_all(
        exchange.reshape(leaf_count * top_count, rhs // 2, 2 * rank),
        ("top", "leaf"),
        0,
        0,
        tiled=True,
    ).reshape(exchange.shape)
    terms = (top_count - 1) + 3 * (coarse - 2) + 2
    levels = leaves.bit_length() - 1
    bf16 = jnp.bfloat16
    path, leaf_path, pair_path, mats, near_pack, coupling_pack = pl.pallas_call(
        prep_kernel,
        out_shape=(
            jax.ShapeDtypeStruct((2, rank, leaves * points), bf16),
            jax.ShapeDtypeStruct((leaves, rank, 2 * points), bf16),
            jax.ShapeDtypeStruct((leaves // 2, (levels - 1) * rank, 4 * points), bf16),
            jax.ShapeDtypeStruct((2, terms * rank, rank), bf16),
            jax.ShapeDtypeStruct((leaves, 3 * points, 2 * points), bf16),
            jax.ShapeDtypeStruct((2 * leaves - 2, 3 * rank, 2 * rank), bf16),
        ),
        in_specs=[vmem] * 4 + [hbm] * 4,
        out_specs=(vmem,) * 6,
        scratch_shapes=[
            pltpu.VMEM(array.shape, f32)
            for array in (coarse_coupling, opposite_coupling, body_coupling, near_blocks)
        ]
        + [pltpu.SemaphoreType.DMA((4,))],
        name="prep",
        compiler_params=params,
        cost_estimate=pl.CostEstimate(flops=20_000_000, bytes_accessed=2_000_000, transcendentals=0),
    )(
        basis_v,
        transfer_v,
        coarse_v,
        coupling_v,
        *stay(coarse_coupling, opposite_coupling, body_coupling, near_blocks),
    )
    known = pl.pallas_call(
        near_kernel,
        out_shape=jax.ShapeDtypeStruct((rhs, leaves * points), f32),
        in_specs=[smem] * 2 + [vmem] * 8,
        out_specs=vmem,
        scratch_shapes=[
            pltpu.VMEM((3 * (2 * leaves - 2), rhs, 2 * rank), f32),
            pltpu.VMEM((leaves + 2 * NEAR, rhs, 2 * points), f32),
        ],
        name="near",
        compiler_params=params,
        cost_estimate=pl.CostEstimate(flops=80_000_000, bytes_accessed=3_000_000, transcendentals=0),
    )(
        jnp.transpose(near_list, (2, 0, 1)),
        jnp.transpose(coupling_list, (2, 0, 1)),
        charges_v,
        near_pack,
        coupling_pack,
        leaf_path,
        pair_path,
        ahead,
        below,
        above,
    )
    return pl.pallas_call(
        final_kernel,
        out_shape=jax.ShapeDtypeStruct(charges.shape, f32),
        in_specs=[vmem] * 5,
        out_specs=vmem,
        scratch_shapes=[
            pltpu.VMEM((leaf_count >> (tier + 1), rhs, rank), f32) for tier in range(coarse - 3)
        ],
        name="final",
        compiler_params=params,
        cost_estimate=pl.CostEstimate(flops=10_000_000, bytes_accessed=600_000, transcendentals=0),
    )(received, known, mats, path, coarse_v)


def solution(mesh):
    in_specs = (
        P("top", None, "leaf"),
        P("top", "leaf", None, None),
        P("top", "leaf", None, None, None),
        P("top", "leaf", None),
        P("top", "leaf", None, None),
        P("top", "leaf", None, None, None),
        P("top", "leaf", None),
        P("top", None, None, None, None),
        P("top", None, None, None, None),
        P("top", None, None),
        P("top", None, None, None),
    )
    out_specs = P("top", None, "leaf")
    return jax.shard_map(
        per_device, mesh=mesh, in_specs=in_specs, out_specs=out_specs, check_vma=False
    )
```

```python
import jax
import jax.numpy as jnp
from jax import lax
from jax.experimental import pallas as pl
from jax.experimental.pallas import tpu as pltpu
from jax.sharding import PartitionSpec as P

NEAR = 4
HIGH = lax.Precision.HIGH
VMEM = pltpu.MemorySpace.VMEM
HBM = pltpu.MemorySpace.HBM


def mm(a, b):
    return lax.dot_general(
        a, b, (((1,), (0,)), ((), ())), precision=HIGH, preferred_element_type=jnp.float32
    )


def mm_t(a, b):
    return lax.dot_general(
        a, b, (((1,), (1,)), ((), ())), precision=HIGH, preferred_element_type=jnp.float32
    )


def halves(x):
    high = x.astype(jnp.bfloat16)
    return high, (x - high.astype(jnp.float32)).astype(jnp.bfloat16)


def packed(x):
    high = x.astype(jnp.bfloat16).astype(jnp.float32)
    return beside(high, x - high).astype(jnp.bfloat16)


def stacked(x):
    high, low = halves(x)
    return jnp.concatenate([high, low], axis=0)


def mm_s(a, b):
    rows = a.shape[0]
    left = stacked(a)
    high, low = halves(b)
    value = dot(left, high)
    return value[:rhs_of(value)] + value[rhs_of(value):] + dot(left[:rows], low)


def rhs_of(value):
    return value.shape[0] // 2


def dot(a, b):
    return lax.dot_general(a, b, (((1,), (0,)), ((), ())), preferred_element_type=jnp.float32)


def beside(a, b):
    return jnp.concatenate([a, b], axis=1)


def unfold(x):
    half = x.shape[1] // 2
    return jnp.concatenate([x[:, :half], x[:, half:]], axis=0)


def tier_span(leaves, height):
    members = leaves >> height
    return 2 * leaves - 2 * members, members


def path_product(coarse_ref, position, tiers):
    product = None
    products = []
    for tier in range(tiers):
        matrix = coarse_ref[0, tier, (position >> tier) & 1]
        product = matrix if product is None else mm(product, matrix)
        products.append(product)
    return products


def fetch(sources, targets, sem):
    copies = [
        pltpu.make_async_copy(source, target, sem.at[i])
        for i, (source, target) in enumerate(zip(sources, targets))
    ]
    for copy in copies:
        copy.start()
    return copies


def up_kernel(
    charges_hbm,
    basis_hbm,
    transfer_hbm,
    coarse_hbm,
    coupling_hbm,
    ahead,
    behind,
    exchange,
    charges,
    basis,
    transfer,
    coarse_transfer,
    coupling,
    sem,
):
    copies = fetch(
        (charges_hbm, basis_hbm, coarse_hbm, transfer_hbm, coupling_hbm),
        (charges, basis, coarse_transfer, transfer, coupling),
        sem,
    )
    leaves, points = basis.shape[1], basis.shape[2]
    levels = leaves.bit_length() - 1
    position = lax.axis_index("leaf")
    body = lax.axis_index("top")
    top_count = exchange.shape[0]
    width = 2 * points
    reach = NEAR * points // width
    whole = leaves // 2
    pairs = leaves - 1
    copies[0].wait()
    copies[1].wait()
    for k in range(reach):
        first = (whole - reach + k) * width
        high = charges[0, :, first : first + width]
        low = charges[0, :, k * width : (k + 1) * width]
        ahead[pairs + k] = high
        behind[pairs + k] = low
    rhs = charges.shape[1]
    low_lanes = lax.broadcasted_iota(jnp.int32, (rhs, width), 1) < points
    coeffs = []
    for j in range(whole):
        pair = charges[0, :, j * width : (j + 1) * width]
        left = jnp.concatenate(
            [jnp.where(low_lanes, pair, 0.0), jnp.where(low_lanes, 0.0, pair)], axis=0
        )
        value = mm_s(left, basis[0, 2 * j : 2 * j + 2].reshape(width, basis.shape[3]))
        coeffs += [value[:rhs], value[rhs:]]
    copies[2].wait()
    copies[3].wait()
    tiers = coarse_transfer.shape[1]
    first, members = tier_span(leaves, levels - 1)
    steps = [coarse_transfer[0, tier, (position >> tier) & 1] for tier in range(tiers)]
    ends = [mm_s(transfer[0, first + n], steps[0]) for n in range(members)]
    rest = beside(steps[-1], steps[-1])
    for step in steps[-2:0:-1]:
        rest = mm_s(step, rest)
    ends = [mm_s(end, rest) for end in ends]
    tops = [beside(transfer[0, first + n], transfer[0, first + n]) for n in range(members)]
    for height in range(levels):
        first, members = tier_span(leaves, height)
        for j in range(members // 2):
            pair = beside(coeffs[2 * j], coeffs[2 * j + 1])
            ahead[first // 2 + j] = pair
            behind[first // 2 + j] = pair
        if height < levels - 1:
            coeffs = [
                mm_s(coeffs[2 * j], transfer[0, first + 2 * j])
                + mm_s(coeffs[2 * j + 1], transfer[0, first + 2 * j + 1])
                for j in range(members // 2)
            ]
    half = rhs // 2

    def doubled(weights):
        value = mm_s(coeffs[0], weights[0]) + mm_s(coeffs[1], weights[1])
        return jnp.where(low_lanes[:half], value[:half], value[half:])

    own = doubled(tops)
    other = doubled(ends)
    for t in range(top_count):
        value = jnp.where(body == t, own, other)
        exchange[t] = jnp.broadcast_to(value[None], (exchange.shape[1],) + value.shape)
    copies[4].wait()


def paths(basis, transfer, path, leaf_path, pair_path):
    leaves, points, rank = basis.shape[1:]
    levels = leaves.bit_length() - 1
    flipped = [basis[0, g].T for g in range(leaves)]
    for g in range(leaves):
        leaf_path[g] = packed(flipped[g])
    wide = [
        beside(*(mm_s(transfer[0, g].T, flipped[g]) for g in (2 * j, 2 * j + 1)))
        for j in range(leaves // 2)
    ]
    width = 2 * points
    for height in range(1, levels):
        first, members = tier_span(leaves, height)
        for j in range(leaves // 2):
            group = leaves // 2 // len(wide)
            at = (j % group) * width
            rows = slice((height - 1) * rank, height * rank)
            pair_path[j, rows, :width], pair_path[j, rows, width:] = halves(
                wide[j // group][:, at : at + width]
            )
        if len(wide) > members:
            wide = [beside(wide[2 * n], wide[2 * n + 1]) for n in range(members)]
        wide = [mm_s(transfer[0, first + n].T, wide[n]) for n in range(members)]
    for n in range(len(wide)):
        size = leaves * points // len(wide)
        columns = slice(n * size, (n + 1) * size)
        path[0, :, columns], path[1, :, columns] = halves(wide[n])


def prep_kernel(
    basis,
    transfer,
    coarse_transfer,
    coupling,
    coarse_coupling_hbm,
    opposite_hbm,
    body_coupling_hbm,
    near_hbm,
    path,
    leaf_path,
    pair_path,
    mats,
    near_pack,
    coupling_pack,
    coarse_coupling,
    opposite,
    body_coupling,
    near_blocks,
    sem,
):
    copies = fetch(
        (coarse_coupling_hbm, opposite_hbm, body_coupling_hbm, near_hbm),
        (coarse_coupling, opposite, body_coupling, near_blocks),
        sem,
    )
    position = lax.axis_index("leaf")


    @pl.when(position >= 0)
    def _():
        paths(basis, transfer, path, leaf_path, pair_path)

    leaves, points, rank = basis.shape[1:]
    coarse = coarse_transfer.shape[1]
    for n in range(2 * leaves - 2):
        coupling_pack[n] = packed(coupling[0, n].reshape(3 * rank, rank))
    products = path_product(coarse_transfer, position, coarse)
    at = 0

    def put(value):
        nonlocal at
        rows = slice(at, at + rank)
        mats[0, rows], mats[1, rows] = halves(value)
        at += rank

    for copy in copies[:3]:
        copy.wait()
    for s in range(body_coupling.shape[1]):
        put(mm_t(body_coupling[0, s], products[coarse - 1]))
    for tier in range(coarse - 2):
        odd = (position >> tier) & 1
        for slot in (1, 2, jnp.where(odd == 1, 0, 3)):
            value = coarse_coupling[0, tier, slot]
            put(value if tier == 0 else mm_t(value, products[tier - 1]))
    far = mm_t(opposite[0], products[coarse - 3])
    put(mm(coarse_transfer[0, coarse - 3, 0], far))
    put(mm(coarse_transfer[0, coarse - 3, 1], far))
    copies[3].wait()
    for g in range(leaves):
        near_pack[g] = packed(near_blocks[0, g].reshape(3 * points, points))


def near_kernel(
    near_list_in,
    coupling_list_in,
    charges,
    near_pack,
    coupling_pack,
    leaf_path,
    pair_path,
    mine,
    below,
    above,
    known,
    window,
    sources,
    near_list,
    coupling_list,
    sem,
):
    copies = fetch((near_list_in, coupling_list_in), (near_list, coupling_list), sem)
    leaves = near_pack.shape[0]
    points = near_pack.shape[2] // 2
    rhs = charges.shape[1]
    levels = leaves.bit_length() - 1
    pairs = leaves - 1
    width = 2 * points
    reach = NEAR * points // width
    low_lanes = lax.broadcasted_iota(jnp.int32, (rhs, width), 1) < points

    def spread(pair, ref, even, odd):
        turned = pltpu.roll(pair, points, 1)
        ref[even] = jnp.where(low_lanes, pair, turned)
        ref[odd] = jnp.where(low_lanes, turned, pair)

    for k in range(reach):
        spread(below[pairs + k], sources, 2 * k, 2 * k + 1)
        at = NEAR + leaves + 2 * k
        spread(above[pairs + k], sources, at, at + 1)
    for k in range(leaves // 2):
        at = NEAR + 2 * k
        spread(charges[0, :, k * width : (k + 1) * width], sources, at, at + 1)
    for height in range(levels):
        first, members = tier_span(leaves, height)
        for block, pack in enumerate((below, mine, above)):
            for j in range(members // 2):
                at = 3 * first + block * members + 2 * j
                spread(pack[first // 2 + j], window, at, at + 1)

    for copy in copies:
        copy.wait()

    def three(a, b, c):
        return beside(jnp.where(low_lanes, a, b), c[:, :points])

    def picked(ref, base, list_ref, n):
        return three(*(ref[base + list_ref[slot, 0, n]] for slot in range(3)))

    def product(left, weights):
        value = dot(stacked(left), weights)
        return value[:rhs] + jnp.where(low_lanes, value[rhs:], 0.0)

    def folded(value):
        return value + pltpu.roll(value, points, 1)

    coupled = []
    for n in range(2 * leaves - 2):
        height = next(h for h in range(levels) if n < sum(tier_span(leaves, h)))
        left = picked(window, 3 * tier_span(leaves, height)[0], coupling_list, n)
        coupled.append(folded(product(left, coupling_pack[n])))
    result = []
    for g in range(leaves):
        value = product(picked(sources, g, near_list, g), near_pack[g])
        result.append(value + product(coupled[g][:, :points], leaf_path[g]))
    for j in range(leaves // 2):
        chain = [coupled[tier_span(leaves, h)[0] + (2 * j >> h)] for h in range(1, levels)]
        left = [
            jnp.where(low_lanes, *chain[h : h + 2]) if h + 1 < len(chain) else chain[h][:, :points]
            for h in range(0, len(chain), 2)
        ]
        value = dot(stacked(jnp.concatenate(left, axis=1)), pair_path[j])
        value = value[:rhs, :width] + value[:rhs, width:] + value[rhs:, :width]
        even, odd = result[2 * j], result[2 * j + 1]
        value = value + jnp.where(low_lanes, even, odd)
        known[:, j * width : (j + 1) * width] = value + pltpu.roll(
            jnp.where(low_lanes, odd, even), points, 1
        )


def final_kernel(received, known, mats, path, coarse_transfer, out, *tier_refs):
    top_count, leaf_count = received.shape[0], received.shape[1]
    coarse = coarse_transfer.shape[1]
    rhs = out.shape[1]
    position = lax.axis_index("leaf")
    body = lax.axis_index("top")
    terms = []
    for s in range(top_count - 1):
        other = lax.rem(body + 1 + s, top_count)
        total = received[other, 0]
        for j in range(1, leaf_count):
            total = total + received[other, j]
        terms.append(unfold(total))

    def node(tier, index):
        if tier == 0:
            return unfold(received[body, index])
        return tier_refs[tier - 1][index]

    for tier in range(coarse - 2):
        count = leaf_count >> tier
        here = position >> tier
        odd = here & 1
        for offset in (-2, 2, jnp.where(odd == 1, -3, 3)):
            terms.append(node(tier, (here + offset + count) & (count - 1)))
        if tier < coarse - 3:
            for j in range(count // 2):
                tier_refs[tier][j] = mm(node(tier, 2 * j), coarse_transfer[0, tier, 0]) + mm(
                    node(tier, 2 * j + 1), coarse_transfer[0, tier, 1]
                )
    across = ((position >> (coarse - 2)) + 2) & 3
    terms.append(node(coarse - 3, 2 * across))
    terms.append(node(coarse - 3, 2 * across + 1))
    left = stacked(jnp.concatenate(terms, axis=1))
    value = dot(left, mats[0])
    left = stacked(value[:rhs] + value[rhs:] + dot(left[:rhs], mats[1]))
    value = dot(left, path[0])
    out[0] = known[...] + value[:rhs] + value[rhs:] + dot(left[:rhs], path[1])


def per_device(
    charges,
    leaf_basis,
    near_blocks,
    near_list,
    local_transfer,
    local_coupling,
    coupling_list,
    coarse_transfer,
    coarse_coupling,
    opposite_coupling,
    body_coupling,
):
    rhs = charges.shape[1]
    leaves, points, rank = leaf_basis.shape[1:]
    leaf_count = lax.axis_size("leaf")
    top_count = lax.axis_size("top")
    coarse = coarse_transfer.shape[1]
    packs = leaves - 1 + NEAR // 2
    f32 = jnp.float32
    vmem = pl.BlockSpec(memory_space=VMEM)
    params = pltpu.CompilerParams(vmem_limit_bytes=8 << 20)
    pack_shape = jax.ShapeDtypeStruct((packs, rhs, 2 * rank), f32)
    hbm = pl.BlockSpec(memory_space=HBM)

    def like(*arrays):
        return tuple(jax.ShapeDtypeStruct(array.shape, array.dtype) for array in arrays)

    def stay(*arrays):
        return [pltpu.with_memory_space_constraint(array, HBM) for array in arrays]

    ahead, behind, exchange, charges_v, basis_v, transfer_v, coarse_v, coupling_v = pl.pallas_call(
        up_kernel,
        out_shape=(
            pack_shape,
            pack_shape,
            jax.ShapeDtypeStruct((top_count, leaf_count, rhs // 2, 2 * rank), f32),
        )
        + like(charges, leaf_basis, local_transfer, coarse_transfer, local_coupling),
        in_specs=[hbm] * 5,
        out_specs=(vmem,) * 8,
        scratch_shapes=[pltpu.SemaphoreType.DMA((5,))],
        name="up",
        compiler_params=params,
        cost_estimate=pl.CostEstimate(flops=40_000_000, bytes_accessed=1_000_000, transcendentals=0),
    )(
        *stay(charges, leaf_basis, local_transfer, coarse_transfer, local_coupling)
    )
    forward = [(i, (i + 1) % leaf_count) for i in range(leaf_count)]
    backward = [(target, source) for source, target in forward]
    below = lax.ppermute(ahead, "leaf", forward)
    above = lax.ppermute(behind, "leaf", backward)
    received = lax.all_to_all(
        exchange.reshape(leaf_count * top_count, rhs // 2, 2 * rank),
        ("top", "leaf"),
        0,
        0,
        tiled=True,
    ).reshape(exchange.shape)
    terms = (top_count - 1) + 3 * (coarse - 2) + 2
    levels = leaves.bit_length() - 1
    bf16 = jnp.bfloat16
    path, leaf_path, pair_path, mats, near_pack, coupling_pack = pl.pallas_call(
        prep_kernel,
        out_shape=(
            jax.ShapeDtypeStruct((2, rank, leaves * points), bf16),
            jax.ShapeDtypeStruct((leaves, rank, 2 * points), bf16),
            jax.ShapeDtypeStruct((leaves // 2, (levels - 1) * rank, 4 * points), bf16),
            jax.ShapeDtypeStruct((2, terms * rank, rank), bf16),
            jax.ShapeDtypeStruct((leaves, 3 * points, 2 * points), bf16),
            jax.ShapeDtypeStruct((2 * leaves - 2, 3 * rank, 2 * rank), bf16),
        ),
        in_specs=[vmem] * 4 + [hbm] * 4,
        out_specs=(vmem,) * 6,
        scratch_shapes=[
            pltpu.VMEM(array.shape, f32)
            for array in (coarse_coupling, opposite_coupling, body_coupling, near_blocks)
        ]
        + [pltpu.SemaphoreType.DMA((4,))],
        name="prep",
        compiler_params=params,
        cost_estimate=pl.CostEstimate(flops=20_000_000, bytes_accessed=2_000_000, transcendentals=0),
    )(
        basis_v,
        transfer_v,
        coarse_v,
        coupling_v,
        *stay(coarse_coupling, opposite_coupling, body_coupling, near_blocks),
    )
    known = pl.pallas_call(
        near_kernel,
        out_shape=jax.ShapeDtypeStruct((rhs, leaves * points), f32),
        in_specs=[vmem] * 10,
        out_specs=vmem,
        scratch_shapes=[
            pltpu.VMEM((3 * (2 * leaves - 2), rhs, 2 * rank), f32),
            pltpu.VMEM((leaves + 2 * NEAR, rhs, 2 * points), f32),
            pltpu.SMEM((near_list.shape[2], 1, leaves), jnp.int32),
            pltpu.SMEM((coupling_list.shape[2], 1, 2 * leaves - 2), jnp.int32),
            pltpu.SemaphoreType.DMA((2,)),
        ],
        name="near",
        compiler_params=params,
        cost_estimate=pl.CostEstimate(flops=80_000_000, bytes_accessed=3_000_000, transcendentals=0),
    )(
        jnp.transpose(near_list, (2, 0, 1)),
        jnp.transpose(coupling_list, (2, 0, 1)),
        charges_v,
        near_pack,
        coupling_pack,
        leaf_path,
        pair_path,
        ahead,
        below,
        above,
    )
    return pl.pallas_call(
        final_kernel,
        out_shape=jax.ShapeDtypeStruct(charges.shape, f32),
        in_specs=[vmem] * 5,
        out_specs=vmem,
        scratch_shapes=[
            pltpu.VMEM((leaf_count >> (tier + 1), rhs, rank), f32) for tier in range(coarse - 3)
        ],
        name="final",
        compiler_params=params,
        cost_estimate=pl.CostEstimate(flops=10_000_000, bytes_accessed=600_000, transcendentals=0),
    )(received, known, mats, path, coarse_v)


def solution(mesh):
    in_specs = (
        P("top", None, "leaf"),
        P("top", "leaf", None, None),
        P("top", "leaf", None, None, None),
        P("top", "leaf", None),
        P("top", "leaf", None, None),
        P("top", "leaf", None, None, None),
        P("top", "leaf", None),
        P("top", None, None, None, None),
        P("top", None, None, None, None),
        P("top", None, None),
        P("top", None, None, None),
    )
    out_specs = P("top", None, "leaf")
    return jax.shard_map(
        per_device, mesh=mesh, in_specs=in_specs, out_specs=out_specs, check_vma=False
    )
```

```python
import jax
import jax.numpy as jnp
from jax import lax
from jax.experimental import pallas as pl
from jax.experimental.pallas import tpu as pltpu
from jax.sharding import PartitionSpec as P

NEAR = 4
HIGH = lax.Precision.HIGH
VMEM = pltpu.MemorySpace.VMEM
HBM = pltpu.MemorySpace.HBM


def mm(a, b):
    return lax.dot_general(
        a, b, (((1,), (0,)), ((), ())), precision=HIGH, preferred_element_type=jnp.float32
    )


def mm_t(a, b):
    return lax.dot_general(
        a, b, (((1,), (1,)), ((), ())), precision=HIGH, preferred_element_type=jnp.float32
    )


def halves(x):
    high = x.astype(jnp.bfloat16)
    return high, (x - high.astype(jnp.float32)).astype(jnp.bfloat16)


def packed(x):
    high = x.astype(jnp.bfloat16).astype(jnp.float32)
    return beside(high, x - high).astype(jnp.bfloat16)


def stacked(x):
    high, low = halves(x)
    return jnp.concatenate([high, low], axis=0)


def mm_s(a, b):
    rows = a.shape[0]
    left = stacked(a)
    high, low = halves(b)
    value = dot(left, high)
    return value[:rhs_of(value)] + value[rhs_of(value):] + dot(left[:rows], low)


def rhs_of(value):
    return value.shape[0] // 2


def dot(a, b):
    return lax.dot_general(a, b, (((1,), (0,)), ((), ())), preferred_element_type=jnp.float32)


def beside(a, b):
    return jnp.concatenate([a, b], axis=1)


def unfold(x):
    half = x.shape[1] // 2
    return jnp.concatenate([x[:, :half], x[:, half:]], axis=0)


def tier_span(leaves, height):
    members = leaves >> height
    return 2 * leaves - 2 * members, members


def path_product(coarse_ref, position, tiers):
    product = None
    products = []
    for tier in range(tiers):
        matrix = coarse_ref[0, tier, (position >> tier) & 1]
        product = matrix if product is None else mm(product, matrix)
        products.append(product)
    return products


def fetch(sources, targets, sem):
    copies = [
        pltpu.make_async_copy(source, target, sem.at[i])
        for i, (source, target) in enumerate(zip(sources, targets))
    ]
    for copy in copies:
        copy.start()
    return copies


def up_kernel(
    charges_hbm,
    basis_hbm,
    transfer_hbm,
    coarse_hbm,
    coupling_hbm,
    ahead,
    behind,
    exchange,
    charges,
    basis,
    transfer,
    coarse_transfer,
    coupling,
    leaf_coeffs,
    sem,
):
    copies = fetch(
        (charges_hbm, basis_hbm, coarse_hbm, transfer_hbm, coupling_hbm),
        (charges, basis, coarse_transfer, transfer, coupling),
        sem,
    )
    leaves, points = basis.shape[1], basis.shape[2]
    levels = leaves.bit_length() - 1
    position = lax.axis_index("leaf")
    body = lax.axis_index("top")
    top_count = exchange.shape[0]
    width = 2 * points
    reach = NEAR * points // width
    whole = leaves // 2
    pairs = leaves - 1
    copies[0].wait()
    copies[1].wait()
    for k in range(reach):
        first = (whole - reach + k) * width
        high = charges[0, :, first : first + width]
        low = charges[0, :, k * width : (k + 1) * width]
        ahead[pairs + k] = high
        behind[pairs + k] = low
    rhs = charges.shape[1]
    low_lanes = lax.broadcasted_iota(jnp.int32, (rhs, width), 1) < points

    @pl.when(position >= 0)
    def _():
        for j in range(whole):
            pair = charges[0, :, j * width : (j + 1) * width]
            left = jnp.concatenate(
                [jnp.where(low_lanes, pair, 0.0), jnp.where(low_lanes, 0.0, pair)], axis=0
            )
            leaf_coeffs[j] = mm_s(left, basis[0, 2 * j : 2 * j + 2].reshape(width, basis.shape[3]))

    coeffs = [leaf_coeffs[g // 2, (g % 2) * rhs : (g % 2 + 1) * rhs] for g in range(leaves)]
    copies[2].wait()
    copies[3].wait()
    tiers = coarse_transfer.shape[1]
    first, members = tier_span(leaves, levels - 1)
    steps = [coarse_transfer[0, tier, (position >> tier) & 1] for tier in range(tiers)]
    ends = [mm_s(transfer[0, first + n], steps[0]) for n in range(members)]
    rest = beside(steps[-1], steps[-1])
    for step in steps[-2:0:-1]:
        rest = mm_s(step, rest)
    ends = [mm_s(end, rest) for end in ends]
    tops = [beside(transfer[0, first + n], transfer[0, first + n]) for n in range(members)]
    for height in range(levels):
        first, members = tier_span(leaves, height)
        for j in range(members // 2):
            pair = beside(coeffs[2 * j], coeffs[2 * j + 1])
            ahead[first // 2 + j] = pair
            behind[first // 2 + j] = pair
        if height < levels - 1:
            coeffs = [
                mm_s(coeffs[2 * j], transfer[0, first + 2 * j])
                + mm_s(coeffs[2 * j + 1], transfer[0, first + 2 * j + 1])
                for j in range(members // 2)
            ]
    half = rhs // 2

    def doubled(weights):
        value = mm_s(coeffs[0], weights[0]) + mm_s(coeffs[1], weights[1])
        return jnp.where(low_lanes[:half], value[:half], value[half:])

    own = doubled(tops)
    other = doubled(ends)
    for t in range(top_count):
        value = jnp.where(body == t, own, other)
        exchange[t] = jnp.broadcast_to(value[None], (exchange.shape[1],) + value.shape)
    copies[4].wait()


def paths(basis, transfer, path, leaf_path, pair_path):
    leaves, points, rank = basis.shape[1:]
    levels = leaves.bit_length() - 1
    flipped = [basis[0, g].T for g in range(leaves)]
    for g in range(leaves):
        leaf_path[g] = packed(flipped[g])
    wide = [
        beside(*(mm_s(transfer[0, g].T, flipped[g]) for g in (2 * j, 2 * j + 1)))
        for j in range(leaves // 2)
    ]
    width = 2 * points
    for height in range(1, levels):
        first, members = tier_span(leaves, height)
        for j in range(leaves // 2):
            group = leaves // 2 // len(wide)
            at = (j % group) * width
            rows = slice((height - 1) * rank, height * rank)
            pair_path[j, rows, :width], pair_path[j, rows, width:] = halves(
                wide[j // group][:, at : at + width]
            )
        if len(wide) > members:
            wide = [beside(wide[2 * n], wide[2 * n + 1]) for n in range(members)]
        wide = [mm_s(transfer[0, first + n].T, wide[n]) for n in range(members)]
    for n in range(len(wide)):
        size = leaves * points // len(wide)
        columns = slice(n * size, (n + 1) * size)
        path[0, :, columns], path[1, :, columns] = halves(wide[n])


def prep_kernel(
    basis,
    transfer,
    coarse_transfer,
    coupling,
    coarse_coupling_hbm,
    opposite_hbm,
    body_coupling_hbm,
    near_hbm,
    path,
    leaf_path,
    pair_path,
    mats,
    near_pack,
    coupling_pack,
    coarse_coupling,
    opposite,
    body_coupling,
    near_blocks,
    sem,
):
    copies = fetch(
        (coarse_coupling_hbm, opposite_hbm, body_coupling_hbm, near_hbm),
        (coarse_coupling, opposite, body_coupling, near_blocks),
        sem,
    )
    position = lax.axis_index("leaf")


    @pl.when(position >= 0)
    def _():
        paths(basis, transfer, path, leaf_path, pair_path)

    leaves, points, rank = basis.shape[1:]
    coarse = coarse_transfer.shape[1]
    for n in range(2 * leaves - 2):
        coupling_pack[n] = packed(coupling[0, n].reshape(3 * rank, rank))
    products = path_product(coarse_transfer, position, coarse)
    at = 0

    def put(value):
        nonlocal at
        rows = slice(at, at + rank)
        mats[0, rows], mats[1, rows] = halves(value)
        at += rank

    for copy in copies[:3]:
        copy.wait()
    for s in range(body_coupling.shape[1]):
        put(mm_t(body_coupling[0, s], products[coarse - 1]))
    for tier in range(coarse - 2):
        odd = (position >> tier) & 1
        for slot in (1, 2, jnp.where(odd == 1, 0, 3)):
            value = coarse_coupling[0, tier, slot]
            put(value if tier == 0 else mm_t(value, products[tier - 1]))
    far = mm_t(opposite[0], products[coarse - 3])
    put(mm(coarse_transfer[0, coarse - 3, 0], far))
    put(mm(coarse_transfer[0, coarse - 3, 1], far))
    copies[3].wait()
    for g in range(leaves):
        near_pack[g] = packed(near_blocks[0, g].reshape(3 * points, points))


def near_kernel(
    near_list_in,
    coupling_list_in,
    charges,
    near_pack,
    coupling_pack,
    leaf_path,
    pair_path,
    mine,
    below,
    above,
    known,
    window,
    sources,
    near_list,
    coupling_list,
    sem,
):
    copies = fetch((near_list_in, coupling_list_in), (near_list, coupling_list), sem)
    leaves = near_pack.shape[0]
    points = near_pack.shape[2] // 2
    rhs = charges.shape[1]
    levels = leaves.bit_length() - 1
    pairs = leaves - 1
    width = 2 * points
    reach = NEAR * points // width
    low_lanes = lax.broadcasted_iota(jnp.int32, (rhs, width), 1) < points

    def spread(pair, ref, even, odd):
        turned = pltpu.roll(pair, points, 1)
        ref[even] = jnp.where(low_lanes, pair, turned)
        ref[odd] = jnp.where(low_lanes, turned, pair)

    for k in range(reach):
        spread(below[pairs + k], sources, 2 * k, 2 * k + 1)
        at = NEAR + leaves + 2 * k
        spread(above[pairs + k], sources, at, at + 1)
    for k in range(leaves // 2):
        at = NEAR + 2 * k
        spread(charges[0, :, k * width : (k + 1) * width], sources, at, at + 1)
    for height in range(levels):
        first, members = tier_span(leaves, height)
        for block, pack in enumerate((below, mine, above)):
            for j in range(members // 2):
                at = 3 * first + block * members + 2 * j
                spread(pack[first // 2 + j], window, at, at + 1)

    for copy in copies:
        copy.wait()

    def three(a, b, c):
        return beside(jnp.where(low_lanes, a, b), c[:, :points])

    def picked(ref, base, list_ref, n):
        return three(*(ref[base + list_ref[slot, 0, n]] for slot in range(3)))

    def product(left, weights):
        value = dot(stacked(left), weights)
        return value[:rhs] + jnp.where(low_lanes, value[rhs:], 0.0)

    def folded(value):
        return value + pltpu.roll(value, points, 1)

    coupled = []
    for n in range(2 * leaves - 2):
        height = next(h for h in range(levels) if n < sum(tier_span(leaves, h)))
        left = picked(window, 3 * tier_span(leaves, height)[0], coupling_list, n)
        coupled.append(folded(product(left, coupling_pack[n])))
    result = []
    for g in range(leaves):
        value = product(picked(sources, g, near_list, g), near_pack[g])
        result.append(value + product(coupled[g][:, :points], leaf_path[g]))
    for j in range(leaves // 2):
        chain = [coupled[tier_span(leaves, h)[0] + (2 * j >> h)] for h in range(1, levels)]
        left = [
            jnp.where(low_lanes, *chain[h : h + 2]) if h + 1 < len(chain) else chain[h][:, :points]
            for h in range(0, len(chain), 2)
        ]
        value = dot(stacked(jnp.concatenate(left, axis=1)), pair_path[j])
        value = value[:rhs, :width] + value[:rhs, width:] + value[rhs:, :width]
        even, odd = result[2 * j], result[2 * j + 1]
        value = value + jnp.where(low_lanes, even, odd)
        known[:, j * width : (j + 1) * width] = value + pltpu.roll(
            jnp.where(low_lanes, odd, even), points, 1
        )


def final_kernel(received, known, mats, path, coarse_transfer, out, *tier_refs):
    top_count, leaf_count = received.shape[0], received.shape[1]
    coarse = coarse_transfer.shape[1]
    rhs = out.shape[1]
    position = lax.axis_index("leaf")
    body = lax.axis_index("top")
    terms = []
    for s in range(top_count - 1):
        other = lax.rem(body + 1 + s, top_count)
        total = received[other, 0]
        for j in range(1, leaf_count):
            total = total + received[other, j]
        terms.append(unfold(total))

    def node(tier, index):
        if tier == 0:
            return unfold(received[body, index])
        return tier_refs[tier - 1][index]

    for tier in range(coarse - 2):
        count = leaf_count >> tier
        here = position >> tier
        odd = here & 1
        for offset in (-2, 2, jnp.where(odd == 1, -3, 3)):
            terms.append(node(tier, (here + offset + count) & (count - 1)))
        if tier < coarse - 3:
            for j in range(count // 2):
                tier_refs[tier][j] = mm(node(tier, 2 * j), coarse_transfer[0, tier, 0]) + mm(
                    node(tier, 2 * j + 1), coarse_transfer[0, tier, 1]
                )
    across = ((position >> (coarse - 2)) + 2) & 3
    terms.append(node(coarse - 3, 2 * across))
    terms.append(node(coarse - 3, 2 * across + 1))
    left = stacked(jnp.concatenate(terms, axis=1))
    value = dot(left, mats[0])
    left = stacked(value[:rhs] + value[rhs:] + dot(left[:rhs], mats[1]))
    value = dot(left, path[0])
    out[0] = known[...] + value[:rhs] + value[rhs:] + dot(left[:rhs], path[1])


def per_device(
    charges,
    leaf_basis,
    near_blocks,
    near_list,
    local_transfer,
    local_coupling,
    coupling_list,
    coarse_transfer,
    coarse_coupling,
    opposite_coupling,
    body_coupling,
):
    rhs = charges.shape[1]
    leaves, points, rank = leaf_basis.shape[1:]
    leaf_count = lax.axis_size("leaf")
    top_count = lax.axis_size("top")
    coarse = coarse_transfer.shape[1]
    packs = leaves - 1 + NEAR // 2
    f32 = jnp.float32
    vmem = pl.BlockSpec(memory_space=VMEM)
    params = pltpu.CompilerParams(vmem_limit_bytes=8 << 20)
    pack_shape = jax.ShapeDtypeStruct((packs, rhs, 2 * rank), f32)
    hbm = pl.BlockSpec(memory_space=HBM)

    def like(*arrays):
        return tuple(jax.ShapeDtypeStruct(array.shape, array.dtype) for array in arrays)

    def stay(*arrays):
        return [pltpu.with_memory_space_constraint(array, HBM) for array in arrays]

    ahead, behind, exchange, charges_v, basis_v, transfer_v, coarse_v, coupling_v = pl.pallas_call(
        up_kernel,
        out_shape=(
            pack_shape,
            pack_shape,
            jax.ShapeDtypeStruct((top_count, leaf_count, rhs // 2, 2 * rank), f32),
        )
        + like(charges, leaf_basis, local_transfer, coarse_transfer, local_coupling),
        in_specs=[hbm] * 5,
        out_specs=(vmem,) * 8,
        scratch_shapes=[
            pltpu.VMEM((leaves // 2, 2 * rhs, rank), f32),
            pltpu.SemaphoreType.DMA((5,)),
        ],
        name="up",
        compiler_params=params,
        cost_estimate=pl.CostEstimate(flops=40_000_000, bytes_accessed=1_000_000, transcendentals=0),
    )(
        *stay(charges, leaf_basis, local_transfer, coarse_transfer, local_coupling)
    )
    forward = [(i, (i + 1) % leaf_count) for i in range(leaf_count)]
    backward = [(target, source) for source, target in forward]
    below = lax.ppermute(ahead, "leaf", forward)
    above = lax.ppermute(behind, "leaf", backward)
    received = lax.all_to_all(
        exchange.reshape(leaf_count * top_count, rhs // 2, 2 * rank),
        ("top", "leaf"),
        0,
        0,
        tiled=True,
    ).reshape(exchange.shape)
    terms = (top_count - 1) + 3 * (coarse - 2) + 2
    levels = leaves.bit_length() - 1
    bf16 = jnp.bfloat16
    path, leaf_path, pair_path, mats, near_pack, coupling_pack = pl.pallas_call(
        prep_kernel,
        out_shape=(
            jax.ShapeDtypeStruct((2, rank, leaves * points), bf16),
            jax.ShapeDtypeStruct((leaves, rank, 2 * points), bf16),
            jax.ShapeDtypeStruct((leaves // 2, (levels - 1) * rank, 4 * points), bf16),
            jax.ShapeDtypeStruct((2, terms * rank, rank), bf16),
            jax.ShapeDtypeStruct((leaves, 3 * points, 2 * points), bf16),
            jax.ShapeDtypeStruct((2 * leaves - 2, 3 * rank, 2 * rank), bf16),
        ),
        in_specs=[vmem] * 4 + [hbm] * 4,
        out_specs=(vmem,) * 6,
        scratch_shapes=[
            pltpu.VMEM(array.shape, f32)
            for array in (coarse_coupling, opposite_coupling, body_coupling, near_blocks)
        ]
        + [pltpu.SemaphoreType.DMA((4,))],
        name="prep",
        compiler_params=params,
        cost_estimate=pl.CostEstimate(flops=20_000_000, bytes_accessed=2_000_000, transcendentals=0),
    )(
        basis_v,
        transfer_v,
        coarse_v,
        coupling_v,
        *stay(coarse_coupling, opposite_coupling, body_coupling, near_blocks),
    )
    known = pl.pallas_call(
        near_kernel,
        out_shape=jax.ShapeDtypeStruct((rhs, leaves * points), f32),
        in_specs=[vmem] * 10,
        out_specs=vmem,
        scratch_shapes=[
            pltpu.VMEM((3 * (2 * leaves - 2), rhs, 2 * rank), f32),
            pltpu.VMEM((leaves + 2 * NEAR, rhs, 2 * points), f32),
            pltpu.SMEM((near_list.shape[2], 1, leaves), jnp.int32),
            pltpu.SMEM((coupling_list.shape[2], 1, 2 * leaves - 2), jnp.int32),
            pltpu.SemaphoreType.DMA((2,)),
        ],
        name="near",
        compiler_params=params,
        cost_estimate=pl.CostEstimate(flops=80_000_000, bytes_accessed=3_000_000, transcendentals=0),
    )(
        jnp.transpose(near_list, (2, 0, 1)),
        jnp.transpose(coupling_list, (2, 0, 1)),
        charges_v,
        near_pack,
        coupling_pack,
        leaf_path,
        pair_path,
        ahead,
        below,
        above,
    )
    return pl.pallas_call(
        final_kernel,
        out_shape=jax.ShapeDtypeStruct(charges.shape, f32),
        in_specs=[vmem] * 5,
        out_specs=vmem,
        scratch_shapes=[
            pltpu.VMEM((leaf_count >> (tier + 1), rhs, rank), f32) for tier in range(coarse - 3)
        ],
        name="final",
        compiler_params=params,
        cost_estimate=pl.CostEstimate(flops=10_000_000, bytes_accessed=600_000, transcendentals=0),
    )(received, known, mats, path, coarse_v)


def solution(mesh):
    in_specs = (
        P("top", None, "leaf"),
        P("top", "leaf", None, None),
        P("top", "leaf", None, None, None),
        P("top", "leaf", None),
        P("top", "leaf", None, None),
        P("top", "leaf", None, None, None),
        P("top", "leaf", None),
        P("top", None, None, None, None),
        P("top", None, None, None, None),
        P("top", None, None),
        P("top", None, None, None),
    )
    out_specs = P("top", None, "leaf")
    return jax.shard_map(
        per_device, mesh=mesh, in_specs=in_specs, out_specs=out_specs, check_vma=False
    )
```
